128 devices in a mesh: gx: 32 (over z_lo, y, x), wa: 4 (over z_hi, core).
Axes of the slice: x: 4, y: 4, z: 4 (z_hi: 2, z_lo: 2; z = z_hi * 2 + z_lo), core: 2. Of those that a mesh axis runs over, the one named last changes fastest.
Arguments:
- warm_field: float32 [64, 2, 512, 2048], P('wa', None, 'gx'), may hold values from -1.8 to 1.8
- warm_adjoint: float32 [64, 2, 512, 2048], P('wa', None, 'gx'), may hold values from -1.8 to 1.8
- permittivity: float32 [512, 2048], P('gx'), may hold values from 1 to 12
- design_mask: int32 [512, 2048], P('gx'), may hold values 0 or 1
- source_row: int32 [64], P('wa'), may hold values from 0 to 511
- monitor_row: int32 [64], P('wa'), may hold values from 0 to 511
- wavenumber: float32 [64], P('wa'), may hold values from 0.02 to 0.08
- bloch_phase: float32 [64], P('wa'), may hold values from -3.140625 to 3.140625
- source_profile: float32 [64, 2, 2048], P('wa'), may hold values from -24 to 24
- monitor_profile: float32 [64, 2, 2048], P('wa'), may hold values from -4 to 4
Outputs:
- forward_field: float32 [64, 2, 512, 2048], P('wa', None, 'gx')
- adjoint_field: float32 [64, 2, 512, 2048], P('wa', None, 'gx')
- gradient: float32 [512, 2048], P('gx')
The draws below stay inside these ranges and needn't reach their ends.
All inputs are finite; a program needn't handle non-finite values. No bound on the sum of `design_mask` on one device may be relied on, other than what follows from the above.
Results may differ from the reference program's by a relative error of at most 0.0003.
Values sent between devices are 32-bit elements; how exact they have to be, the bound alone decides.
No kernel may reach another device: no remote copies, remote signals or barrier semaphores. Data moves between devices by JAX's collectives and lax.ppermute only.
A program may use at most 128 MiB of HBM per device.

```python
import math
import jax
import jax.numpy as jnp
from jax import lax

NY = 2048
NX = 512
WAVES = 64


rough_amp = 0.01


smooth_amp = 0.3


noise_share = 0.005


def wave_kinds(key):
    ranking = jax.random.permutation(jax.random.fold_in(key, 5), WAVES)
    return ranking < max(1, WAVES // 4)


def rough_start(key):
    key_base, key_rows, key_cols = jax.random.split(key, 3)
    position = jnp.arange(NX, dtype=jnp.float32) / NX
    jitter = jax.random.uniform(key_rows, (NX,), jnp.float32, -0.15, 0.15)
    row_scale = jnp.exp(math.log(10.0) * jnp.clip(position + jitter, 0.0, 1.0))
    col_scale = jnp.exp(jax.random.uniform(key_cols, (NY,), jnp.float32, 0.0, math.log(3.0)))
    texture = jnp.clip(jax.random.normal(key_base, (WAVES, 2, NX, NY), jnp.float32), -6.0, 6.0)
    return rough_amp * texture * row_scale[:, None] * col_scale


def smooth_start(key):
    key_rotation, key_rough = jax.random.split(key)
    along_x = jnp.sin(math.pi * (jnp.arange(NX, dtype=jnp.float32) + 0.5) / NX)
    along_y = jnp.sin(math.pi * (jnp.arange(NY, dtype=jnp.float32) + 1.0) / (NY + 1))
    rotation = jax.random.uniform(key_rotation, (WAVES,), jnp.float32, -math.pi, math.pi)
    phasor = jnp.stack([jnp.cos(rotation), jnp.sin(rotation)], axis=1)
    envelope = along_x[:, None] * along_y[None, :]
    roughness = jnp.clip(jax.random.normal(key_rough, (WAVES, 2, NX, NY), jnp.float32), -6.0, 6.0)
    return smooth_amp * (phasor[:, :, None, None] * envelope + noise_share * roughness)


def blended_start(key, stream_salt):
    own_key = jax.random.fold_in(key, stream_salt)
    smooth_kind = wave_kinds(key)
    return jnp.where(smooth_kind[:, None, None, None], smooth_start(jax.random.fold_in(own_key, 1)), rough_start(jax.random.fold_in(own_key, 2)))


def profile_draw(key, stream_salt, scale, bound, weak):
    own_key = jax.random.fold_in(key, stream_salt)
    smooth_kind = wave_kinds(key)
    texture = jnp.clip(jax.random.normal(own_key, (WAVES, 2, NY), jnp.float32), -bound, bound)
    weight = jnp.where(smooth_kind, weak, 1.0)
    return scale * weight[:, None, None] * texture


def draw_warm_field(key, part):
    return blended_start(key, 11)


def draw_warm_adjoint(key, part):
    return blended_start(key, 23)


def draw_source_profile(key, part):
    return profile_draw(key, 31, 4.0, 6.0, 0.004)


def draw_monitor_profile(key, part):
    return profile_draw(key, 37, 1.0, 4.0, 0.02)


def place_ends(result, rng, least, top_value):
    shape = result.shape
    place = [jax.random.randint(jax.random.fold_in(rng, axis), (), 0, shape[axis]) for axis in range(len(shape))]
    result = result.at[tuple(place)].set(least)
    longest = shape.index(max(shape))
    place[longest] = (place[longest] + 1) % shape[longest]
    return result.at[tuple(place)].set(top_value)


def shard_levels(key, dims, shards, smallest, top_value):
    gain = 1.0
    for dim, parts in shards:
        heights = jax.random.uniform(jax.random.fold_in(jax.random.fold_in(key, 6), dim), (parts,), jnp.float32, smallest / len(shards), top_value / len(shards))
        gain = gain * jnp.repeat(jnp.exp(heights), dims[dim] // parts).reshape((-1,) + (1,) * (len(dims) - 1 - dim))
    return gain


def setup_inputs(seed: int = 0) -> dict:
    key_list = jax.random.split(jax.random.key(seed), 11)
    warm_field = draw_warm_field(jax.random.fold_in(key_list[10], 71), 0)
    warm_adjoint = draw_warm_adjoint(jax.random.fold_in(key_list[10], 71), 0)
    permittivity = jnp.clip(1.0 + 11.0 * jax.random.uniform(key_list[2], (NX, NY), jnp.float32) ** shard_levels(key_list[2], (NX, NY), ((0, 32),), -0.2, 0.2), 1.0, 12.0)
    design_mask = place_ends((jax.random.randint(key_list[3], (NX, NY), 0, 2) < 1).astype(jnp.int32), jax.random.fold_in(key_list[3], 1), 0, 1)
    source_row = place_ends(jax.random.randint(key_list[4], (WAVES,), 0, NX), jax.random.fold_in(key_list[4], 1), 0, NX - 1).astype(jnp.int32)
    monitor_row = place_ends(jax.random.randint(key_list[5], (WAVES,), 0, NX), jax.random.fold_in(key_list[5], 1), 0, NX - 1).astype(jnp.int32)
    wavenumber = jnp.clip(jnp.exp(math.log(0.08) - 1.3862944 * jax.random.uniform(key_list[6], (WAVES,), jnp.float32) ** shard_levels(key_list[6], (WAVES,), ((0, 4),), -0.2, 0.2)), 0.02, 0.08)
    bloch_phase = jnp.clip(jax.random.uniform(key_list[7], (WAVES,), jnp.float32, -3.140625, 3.140625), -3.140625, 3.140625)
    source_profile = draw_source_profile(jax.random.fold_in(key_list[10], 71), 0)
    monitor_profile = draw_monitor_profile(jax.random.fold_in(key_list[10], 71), 0)
    return dict(warm_field=warm_field, warm_adjoint=warm_adjoint, permittivity=permittivity, design_mask=design_mask, source_row=source_row, monitor_row=monitor_row, wavenumber=wavenumber, bloch_phase=bloch_phase, source_profile=source_profile, monitor_profile=monitor_profile)


floor_share = 0.5


def rotate(part, cosine, sine):
    return jnp.stack([cosine * part[0] - sine * part[1], sine * part[0] + cosine * part[1]])


def operate(field, diagonal, cosine, sine):
    above = jnp.concatenate([field[:, 1:], rotate(field[:, :1], cosine, sine)], axis=1)
    below = jnp.concatenate([rotate(field[:, -1:], cosine, -sine), field[:, :-1]], axis=1)
    zero_col = jnp.zeros_like(field[..., :1])
    y_after = jnp.concatenate([field[..., 1:], zero_col], axis=-1)
    y_before = jnp.concatenate([zero_col, field[..., :-1]], axis=-1)
    return diagonal * field - (above + below + y_after + y_before)


def complex_scale(scale_re, scale_im, vector):
    return jnp.stack([scale_re * vector[0] - scale_im * vector[1], scale_re * vector[1] + scale_im * vector[0]])


def solve_step(right_side, initial, diagonal, cosine, sine):
    residual = right_side - operate(initial, diagonal, cosine, sine)
    res_norm = jnp.sum(residual * residual)
    precond = residual / diagonal
    image = operate(precond, diagonal, cosine, sine)
    dot_re = jnp.sum(residual[0] * image[0] + residual[1] * image[1])
    dot_im = jnp.sum(residual[0] * image[1] - residual[1] * image[0])
    bounded = jnp.maximum(dot_re * dot_re + dot_im * dot_im, (floor_share * res_norm) * (floor_share * res_norm))
    step_re = res_norm * dot_re / bounded
    step_im = -res_norm * dot_im / bounded
    shrunk = residual - complex_scale(step_re, step_im, image)
    second = shrunk / diagonal
    turned = operate(second, diagonal, cosine, sine)
    ts_re = jnp.sum(turned[0] * shrunk[0] + turned[1] * shrunk[1])
    ts_im = jnp.sum(turned[0] * shrunk[1] - turned[1] * shrunk[0])
    tt_sum = jnp.sum(turned * turned)
    omega_re = ts_re / tt_sum
    omega_im = ts_im / tt_sum
    return initial + complex_scale(step_re, step_im, precond) + complex_scale(omega_re, omega_im, second)


def reference(warm_field, warm_adjoint, permittivity, design_mask, source_row, monitor_row, wavenumber, bloch_phase, source_profile, monitor_profile):
    row_index = jnp.arange(NX)

    def per_wave(running, packed):
        start_fwd, start_adj, src_at, mon_at, squared_k, phase_angle, src_prof, mon_prof = packed
        diagonal = 4.0 - squared_k * permittivity
        cosine = jnp.cos(phase_angle)
        sine = jnp.sin(phase_angle)
        src_sel = (row_index == src_at).astype(jnp.float32)[None, :, None]
        right_side = src_sel * src_prof[:, None, :]
        forward = solve_step(right_side, start_fwd, diagonal, cosine, sine)
        mon_sel = (row_index == mon_at).astype(jnp.float32)
        mon_vals = jnp.sum(mon_sel[None, :, None] * forward, axis=1)
        over_re = jnp.sum(mon_prof[0] * mon_vals[0] + mon_prof[1] * mon_vals[1])
        over_im = jnp.sum(mon_prof[0] * mon_vals[1] - mon_prof[1] * mon_vals[0])
        adj_re = over_re * mon_prof[0] - over_im * mon_prof[1]
        adj_im = -(over_re * mon_prof[1] + over_im * mon_prof[0])
        adj_side = mon_sel[None, :, None] * jnp.stack([adj_re, adj_im])[:, None, :]
        adjoint = solve_step(adj_side, start_adj, diagonal, cosine, -sine)
        contrib = 2.0 * squared_k * (adjoint[0] * forward[0] - adjoint[1] * forward[1])
        return running + contrib, (forward, adjoint)

    summed_init = jnp.zeros((NX, NY), jnp.float32)
    summed, outputs = lax.scan(per_wave, summed_init, (warm_field, warm_adjoint, source_row, monitor_row, wavenumber, bloch_phase, source_profile, monitor_profile))
    gradient = design_mask.astype(jnp.float32) * summed
    return outputs[0], outputs[1], gradient
```

```python
import functools

import jax
import jax.numpy as jnp
from jax import lax
from jax.experimental import pallas as pl
from jax.experimental.pallas import tpu as pltpu
from jax.sharding import PartitionSpec as P

floor_share = 0.5
LANES = 128
SUBLANES = 8
HALO = 3
N_SUMS = 15


def pack_kernel(field_ref, rows_ref, head_ref, tail_ref):
    waves, parts, rows, width = field_ref.shape
    for part in range(parts):
        for wave0 in range(0, waves, SUBLANES):
            for row0 in range(0, rows, SUBLANES):
                for lane0 in range(0, width, LANES):
                    lanes = slice(lane0, lane0 + LANES)
                    block = field_ref[
                        wave0 : wave0 + SUBLANES, part, row0 : row0 + SUBLANES, lanes
                    ]
                    turned = jnp.swapaxes(block, 0, 1)
                    rows_ref[
                        row0 : row0 + SUBLANES, part, wave0 : wave0 + SUBLANES, lanes
                    ] = turned
                    for k in range(HALO):
                        if row0 <= k < row0 + SUBLANES:
                            head_ref[k, part, wave0 : wave0 + SUBLANES, lanes] = turned[k - row0]
                        last = rows - HALO + k
                        if row0 <= last < row0 + SUBLANES:
                            tail_ref[k, part, wave0 : wave0 + SUBLANES, lanes] = turned[last - row0]


def packed(field):
    waves, parts, rows, width = field.shape
    chunk = 256
    shapes = [
        jax.ShapeDtypeStruct((n, parts, waves, width), field.dtype) for n in (rows, HALO, HALO)
    ]
    return pl.pallas_call(
        pack_kernel,
        grid=(width // chunk,),
        in_specs=[pl.BlockSpec((waves, parts, rows, chunk), lambda j: (0, 0, 0, j))],
        out_specs=[
            pl.BlockSpec((s.shape[0], parts, waves, chunk), lambda j: (0, 0, 0, j)) for s in shapes
        ],
        out_shape=shapes,
        name="pack_rows",
    )(field)


def lane_neighbours(load, count):
    lane = lax.broadcasted_iota(jnp.int32, (SUBLANES, LANES), 1)
    at_low = lane == 0
    at_high = lane == LANES - 1
    zero = jnp.zeros((SUBLANES, LANES), jnp.float32)
    tile = load(0)
    up_before = zero
    down_here = pltpu.roll(tile, LANES - 1, 1)
    for j in range(count):
        up_here = pltpu.roll(tile, 1, 1)
        if j + 1 < count:
            following = load(j + 1)
            down_after = pltpu.roll(following, LANES - 1, 1)
        else:
            following, down_after = None, zero
        yield (
            j,
            tile,
            jnp.where(at_low, up_before, up_here) + jnp.where(at_high, down_after, down_here),
        )
        tile, up_before, down_here = following, up_here, down_after


def solve_kernel(
    first_row_ref,
    side_row_ref,
    mark_row_ref,
    rows_hbm,
    above_hbm,
    below_hbm,
    eps_ref,
    wave_ref,
    side_ref,
    mark_ref,
    precond_hbm,
    scaled_hbm,
    sums_ref,
    x_ref,
    z_ref,
    u_ref,
    inv_ref,
    mark_sums,
    sems,
    *,
    conjugate_side,
    total_rows,
):
    rows, parts, waves, width = rows_hbm.shape
    tiles = width // LANES
    loads = [
        pltpu.make_async_copy(above_hbm, x_ref.at[pl.ds(0, HALO)], sems.at[0]),
        pltpu.make_async_copy(rows_hbm, x_ref.at[pl.ds(HALO, rows)], sems.at[1]),
        pltpu.make_async_copy(below_hbm, x_ref.at[pl.ds(HALO + rows, HALO)], sems.at[2]),
    ]
    for copy in loads:
        copy.start()
    mark_sums[...] = jnp.zeros_like(mark_sums)
    for copy in loads:
        copy.wait()
    first_row = first_row_ref[0]

    def wave_column(index, wave0):
        return jnp.broadcast_to(
            wave_ref[wave0 : wave0 + SUBLANES, index : index + 1], (SUBLANES, LANES)
        )

    def any_at(table_ref, row):
        hit = table_ref[0] == row
        for w in range(1, waves):
            hit = jnp.logical_or(hit, table_ref[w] == row)
        return hit

    for wave0 in range(0, waves, SUBLANES):
        group = slice(wave0, wave0 + SUBLANES)
        for base, offset in ((0, 1), (HALO + rows, 3)):
            cosine = wave_column(offset, wave0)
            sine = wave_column(offset + 1, wave0)
            for k in range(HALO):
                for j in range(tiles):
                    lanes = slice(j * LANES, (j + 1) * LANES)
                    re = x_ref[base + k, 0, group, lanes]
                    im = x_ref[base + k, 1, group, lanes]
                    x_ref[base + k, 0, group, lanes] = cosine * re - sine * im
                    x_ref[base + k, 1, group, lanes] = sine * re + cosine * im

    def diagonal_at(eps_row, j, squared_k):
        eps = eps_ref[eps_row, :, j * LANES : (j + 1) * LANES]
        return 4.0 - squared_k * jnp.broadcast_to(eps, (SUBLANES, LANES))

    def residual_row(i, _):
        for wave0 in range(0, waves, SUBLANES):
            group = slice(wave0, wave0 + SUBLANES)
            squared_k = wave_column(0, wave0)
            diagonals = []
            for part in range(parts):
                load = lambda j: x_ref[i + 1, part, group, j * LANES : (j + 1) * LANES]
                for j, centre, sides in lane_neighbours(load, tiles):
                    lanes = slice(j * LANES, (j + 1) * LANES)
                    if part == 0:
                        diagonal = diagonal_at(i, j, squared_k)
                        inverse = 1.0 / diagonal
                        inv_ref[i, group, lanes] = inverse
                    else:
                        diagonal = diagonal_at(i, j, squared_k)
                        inverse = inv_ref[i, group, lanes]
                    around = x_ref[i, part, group, lanes] + x_ref[i + 2, part, group, lanes]
                    z_ref[i, part, group, lanes] = (around + sides - diagonal * centre) * inverse
        row = first_row + i - 2
        row = jnp.where(row < 0, row + total_rows, row)
        row = jnp.where(row >= total_rows, row - total_rows, row)

        @pl.when(any_at(side_row_ref, row))
        def _():
            for wave0 in range(0, waves, SUBLANES):
                group = slice(wave0, wave0 + SUBLANES)
                low = wave_column(1, wave0), wave_column(2, wave0)
                high = wave_column(3, wave0), wave_column(4, wave0)
                cosine = jnp.where(i < 2, low[0], jnp.where(i >= rows + 2, high[0], 1.0))
                sine = jnp.where(i < 2, low[1], jnp.where(i >= rows + 2, high[1], 0.0))
                column = 5 if not conjugate_side else 6
                chosen = wave_column(column, wave0) == row.astype(jnp.float32)
                for j in range(tiles):
                    lanes = slice(j * LANES, (j + 1) * LANES)
                    re = side_ref[group, 0, lanes]
                    im = side_ref[group, 1, lanes]
                    if conjugate_side:
                        over_re = wave_column(7, wave0)
                        over_im = wave_column(8, wave0)
                        re, im = over_re * re - over_im * im, -(over_re * im + over_im * re)
                    inverse = inv_ref[i, group, lanes]
                    z_ref[i, 0, group, lanes] += jnp.where(
                        chosen, (cosine * re - sine * im) * inverse, 0.0
                    )
                    z_ref[i, 1, group, lanes] += jnp.where(
                        chosen, (sine * re + cosine * im) * inverse, 0.0
                    )

        return 0

    lax.fori_loop(0, rows + 4, residual_row, 0)
    store_z = pltpu.make_async_copy(z_ref.at[pl.ds(2, rows)], precond_hbm, sems.at[3])
    store_z.start()

    def image_row(i, _):
        for wave0 in range(0, waves, SUBLANES):
            group = slice(wave0, wave0 + SUBLANES)
            squared_k = wave_column(0, wave0)
            for part in range(parts):
                load = lambda j: z_ref[i + 1, part, group, j * LANES : (j + 1) * LANES]
                for j, centre, sides in lane_neighbours(load, tiles):
                    lanes = slice(j * LANES, (j + 1) * LANES)
                    around = z_ref[i, part, group, lanes] + z_ref[i + 2, part, group, lanes]
                    image = diagonal_at(i + 1, j, squared_k) * centre - (around + sides)
                    u_ref[i, part, group, lanes] = image * inv_ref[i + 1, group, lanes]
        return 0

    lax.fori_loop(0, rows + 2, image_row, 0)
    store_u = pltpu.make_async_copy(u_ref.at[pl.ds(1, rows)], scaled_hbm, sems.at[4])
    store_u.start()

    lane = lax.broadcasted_iota(jnp.int32, (SUBLANES, LANES), 1)
    for wave0 in range(0, waves, SUBLANES):
        group = slice(wave0, wave0 + SUBLANES)

        def twice_row(i, sums, wave0=wave0, group=group):
            squared_k = wave_column(0, wave0)
            rr, rv_re, rv_im, vv, wr_re, wr_im, wv_re, wv_im, ww = sums
            both = [
                lane_neighbours(
                    lambda j, part=part: u_ref[i + 1, part, group, j * LANES : (j + 1) * LANES],
                    tiles,
                )
                for part in range(parts)
            ]
            for (j, u_re, sides_re), (_, u_im, sides_im) in zip(*both):
                lanes = slice(j * LANES, (j + 1) * LANES)
                diagonal = diagonal_at(i + 2, j, squared_k)
                r_re = diagonal * z_ref[i + 2, 0, group, lanes]
                r_im = diagonal * z_ref[i + 2, 1, group, lanes]
                v_re = diagonal * u_re
                v_im = diagonal * u_im
                w_re = v_re - (
                    u_ref[i, 0, group, lanes] + u_ref[i + 2, 0, group, lanes] + sides_re
                )
                w_im = v_im - (
                    u_ref[i, 1, group, lanes] + u_ref[i + 2, 1, group, lanes] + sides_im
                )
                rr += r_re * r_re + r_im * r_im
                rv_re += r_re * v_re + r_im * v_im
                rv_im += r_re * v_im - r_im * v_re
                vv += v_re * v_re + v_im * v_im
                wr_re += w_re * r_re + w_im * r_im
                wr_im += w_re * r_im - w_im * r_re
                wv_re += w_re * v_re + w_im * v_im
                wv_im += w_re * v_im - w_im * v_re
                ww += w_re * w_re + w_im * w_im
            return rr, rv_re, rv_im, vv, wr_re, wr_im, wv_re, wv_im, ww

        zero = jnp.zeros((SUBLANES, LANES), jnp.float32)
        sums = list(lax.fori_loop(0, rows, twice_row, (zero,) * 9))
        if not conjugate_side:

            def mark_at(i, _, wave0=wave0, group=group):
                row = first_row + i

                @pl.when(any_at(mark_row_ref, row))
                def _():
                    chosen = wave_column(6, wave0) == row.astype(jnp.float32)
                    for j in range(tiles):
                        lanes = slice(j * LANES, (j + 1) * LANES)
                        m_re = jnp.where(chosen, mark_ref[group, 0, lanes], 0.0)
                        m_im = jnp.where(chosen, mark_ref[group, 1, lanes], 0.0)
                        for n, (ref, at) in enumerate(((x_ref, 3), (z_ref, 2), (u_ref, 1))):
                            f_re = ref[i + at, 0, group, lanes]
                            f_im = ref[i + at, 1, group, lanes]
                            mark_sums[2 * n, group] += m_re * f_re + m_im * f_im
                            mark_sums[2 * n + 1, group] += m_re * f_im - m_im * f_re

                return 0

            lax.fori_loop(0, rows, mark_at, 0)
            sums += [mark_sums[n, group] for n in range(6)]
        out = zero
        for n, total in enumerate(sums):
            out = jnp.where(lane == n, jnp.sum(total, axis=1, keepdims=True), out)
        sums_ref[group, :] = out
    store_z.wait()
    store_u.wait()


def solve(
    packed_rows, above, below, eps_ext, waves_table, tables, side, mark, conjugate_side, total_rows
):
    rows, parts, waves, width = packed_rows.shape
    hbm = pl.BlockSpec(memory_space=pl.ANY)
    smem = pl.BlockSpec(memory_space=pltpu.SMEM)
    vmem = pl.BlockSpec(memory_space=pltpu.VMEM)
    shape = jax.ShapeDtypeStruct(packed_rows.shape, jnp.float32)
    return pl.pallas_call(
        functools.partial(solve_kernel, conjugate_side=conjugate_side, total_rows=total_rows),
        in_specs=[smem, smem, smem, hbm, hbm, hbm, vmem, vmem, vmem, vmem],
        out_specs=[hbm, hbm, vmem],
        out_shape=[shape, shape, jax.ShapeDtypeStruct((waves, LANES), jnp.float32)],
        scratch_shapes=[
            pltpu.VMEM((rows + 6, parts, waves, width), jnp.float32),
            pltpu.VMEM((rows + 4, parts, waves, width), jnp.float32),
            pltpu.VMEM((rows + 2, parts, waves, width), jnp.float32),
            pltpu.VMEM((rows + 4, waves, width), jnp.float32),
            pltpu.VMEM((6, waves, LANES), jnp.float32),
            pltpu.SemaphoreType.DMA((5,)),
        ],
        compiler_params=pltpu.CompilerParams(vmem_limit_bytes=40 * 2**20),
        name="adjoint_solve" if conjugate_side else "forward_solve",
    )(*tables, packed_rows, above, below, eps_ext, waves_table, side, mark)


def finish_kernel(
    coef_ref, xf_ref, zf_ref, uf_ref, xa_ref, za_ref, ua_ref, fwd_ref, adj_ref, grad_ref
):
    rows, parts, waves, width = xf_ref.shape

    def column(index, wave0):
        return jnp.broadcast_to(
            coef_ref[wave0 : wave0 + SUBLANES, index : index + 1], (SUBLANES, LANES)
        )

    sublane = lax.broadcasted_iota(jnp.int32, (SUBLANES, LANES), 0)
    for lane0 in range(0, width, LANES):
        lanes = slice(lane0, lane0 + LANES)
        for row0 in range(0, rows, SUBLANES):
            terms = [jnp.zeros((SUBLANES, LANES), jnp.float32)] * SUBLANES
            for wave0 in range(0, waves, SUBLANES):
                group = slice(wave0, wave0 + SUBLANES)
                coefs = [column(n, wave0) for n in range(9)]
                results = [[], [], [], []]
                for k in range(SUBLANES):
                    row = row0 + k
                    values = []
                    for base, x_ref, z_ref, u_ref in (
                        (0, xf_ref, zf_ref, uf_ref),
                        (4, xa_ref, za_ref, ua_ref),
                    ):
                        a_re, a_im, b_re, b_im = coefs[base : base + 4]
                        z_re, z_im = z_ref[row, 0, group, lanes], z_ref[row, 1, group, lanes]
                        u_re, u_im = u_ref[row, 0, group, lanes], u_ref[row, 1, group, lanes]
                        values.append(
                            x_ref[row, 0, group, lanes]
                            + (a_re * z_re - a_im * z_im)
                            + (b_re * u_re - b_im * u_im)
                        )
                        values.append(
                            x_ref[row, 1, group, lanes]
                            + (a_re * z_im + a_im * z_re)
                            + (b_re * u_im + b_im * u_re)
                        )
                    f_re, f_im, a_re, a_im = values
                    terms[k] = terms[k] + coefs[8] * (a_re * f_re - a_im * f_im)
                    for n in range(4):
                        results[n].append(values[n])
                for n, (ref, part) in enumerate(
                    ((fwd_ref, 0), (fwd_ref, 1), (adj_ref, 0), (adj_ref, 1))
                ):
                    ref[group, part, row0 : row0 + SUBLANES, lanes] = jnp.swapaxes(
                        jnp.stack(results[n]), 0, 1
                    )
            out = jnp.zeros((SUBLANES, LANES), jnp.float32)
            for k in range(SUBLANES):
                out = jnp.where(sublane == k, jnp.sum(terms[k], axis=0, keepdims=True), out)
            grad_ref[row0 : row0 + SUBLANES, lanes] = out


def finish(coefs, forward_parts, adjoint_parts):
    rows, parts, waves, width = forward_parts[0].shape
    chunk = 128
    packed_spec = pl.BlockSpec((rows, parts, waves, chunk), lambda j: (0, 0, 0, j))
    field_spec = pl.BlockSpec((waves, parts, rows, chunk), lambda j: (0, 0, 0, j))
    field = jax.ShapeDtypeStruct((waves, parts, rows, width), jnp.float32)
    return pl.pallas_call(
        finish_kernel,
        grid=(width // chunk,),
        in_specs=[pl.BlockSpec((waves, LANES), lambda j: (0, 0))] + [packed_spec] * 6,
        out_specs=[field_spec, field_spec, pl.BlockSpec((rows, chunk), lambda j: (0, j))],
        out_shape=[field, field, jax.ShapeDtypeStruct((rows, width), jnp.float32)],
        name="finish",
    )(coefs, *forward_parts, *adjoint_parts)


def over_copies(sums, axis):
    size = lax.axis_size(axis)
    flat = sums[:, :N_SUMS].reshape(1, -1)
    everything = lax.all_to_all(
        jnp.broadcast_to(flat[None], (size, *flat.shape)), axis, 0, 0, tiled=True
    )
    return jnp.sum(everything, axis=0).reshape(sums.shape[0], N_SUMS)


def step_lengths(summed):
    rr, rv_re, rv_im, vv, wr_re, wr_im, wv_re, wv_im, ww = (summed[:, n] for n in range(9))
    half = floor_share * rr
    bounded = jnp.maximum(rv_re * rv_re + rv_im * rv_im, half * half)
    a_re = rr * rv_re / bounded
    a_im = -rr * rv_im / bounded
    a_sq = a_re * a_re + a_im * a_im
    ts_re = rv_re - a_re * vv - (a_re * wr_re + a_im * wr_im) + a_sq * wv_re
    ts_im = -rv_im - a_im * vv - (a_re * wr_im - a_im * wr_re) + a_sq * wv_im
    tt = vv - 2.0 * (a_re * wv_re + a_im * wv_im) + a_sq * ww
    o_re = ts_re / tt
    o_im = ts_im / tt
    return (a_re + o_re, a_im + o_im, a_im * o_im - a_re * o_re, -(a_re * o_im + a_im * o_re))


def table_of(columns, count=LANES):
    waves = columns[0].shape[0]
    stacked = jnp.stack(columns, axis=1)
    return jnp.pad(stacked, ((0, 0), (0, count - len(columns))))


def local(
    warm_field,
    warm_adjoint,
    permittivity,
    design_mask,
    source_row,
    monitor_row,
    wavenumber,
    bloch_phase,
    source_profile,
    monitor_profile,
):
    rows = permittivity.shape[0]
    count = lax.axis_size("gx")
    index = lax.axis_index("gx")
    up = [(i, (i + 1) % count) for i in range(count)]
    down = [((i + 1) % count, i) for i in range(count)]
    eps_above = lax.ppermute(permittivity[-2:], "gx", up)
    eps_below = lax.ppermute(permittivity[:2], "gx", down)
    fwd_rows, fwd_head, fwd_tail = packed(warm_field)
    fwd_above = lax.ppermute(fwd_tail, "gx", up)
    fwd_below = lax.ppermute(fwd_head, "gx", down)
    adj_rows, adj_head, adj_tail = packed(warm_adjoint)
    adj_above = lax.ppermute(adj_tail, "gx", up)
    adj_below = lax.ppermute(adj_head, "gx", down)
    eps_ext = jnp.concatenate(
        [eps_above, permittivity, eps_below], axis=0
    )[:, None, :]
    at_first = index == 0
    at_last = index == count - 1
    cosine = jnp.cos(bloch_phase)
    sine = jnp.sin(bloch_phase)
    one = jnp.ones_like(cosine)
    zero = jnp.zeros_like(cosine)
    row_columns = [source_row.astype(jnp.float32), monitor_row.astype(jnp.float32)]
    first_row = (index * rows).astype(jnp.int32).reshape(1)

    def rotation(sign):
        return [
            jnp.where(at_first, cosine, one),
            jnp.where(at_first, -sign * sine, zero),
            jnp.where(at_last, cosine, one),
            jnp.where(at_last, sign * sine, zero),
        ]

    tables = (first_row, source_row, monitor_row)
    fwd_z, fwd_u, fwd_sums = solve(
        fwd_rows,
        fwd_above,
        fwd_below,
        eps_ext,
        table_of([wavenumber] + rotation(1.0) + row_columns),
        tables,
        source_profile,
        monitor_profile,
        False,
        rows * count,
    )
    summed = over_copies(fwd_sums, "gx")
    fwd_coefs = step_lengths(summed)
    a_re, a_im, b_re, b_im = fwd_coefs
    s0_re, s0_im, s1_re, s1_im, s2_re, s2_im = (summed[:, n] for n in range(9, 15))
    over_re = s0_re + (a_re * s1_re - a_im * s1_im) + (b_re * s2_re - b_im * s2_im)
    over_im = s0_im + (a_re * s1_im + a_im * s1_re) + (b_re * s2_im + b_im * s2_re)
    adj_z, adj_u, adj_sums = solve(
        adj_rows,
        adj_above,
        adj_below,
        eps_ext,
        table_of([wavenumber] + rotation(-1.0) + row_columns + [over_re, over_im]),
        (first_row, monitor_row, monitor_row),
        monitor_profile,
        monitor_profile,
        True,
        rows * count,
    )
    adj_coefs = step_lengths(over_copies(adj_sums, "gx"))
    forward, adjoint, partial = finish(
        table_of(list(fwd_coefs) + list(adj_coefs) + [2.0 * wavenumber]),
        (fwd_rows, fwd_z, fwd_u),
        (adj_rows, adj_z, adj_u),
    )
    summed_terms = lax.all_gather(partial, "wa").sum(axis=0)
    gradient = design_mask.astype(jnp.float32) * summed_terms
    return (forward, adjoint, gradient)


def solution(mesh):
    placed = (
        P("wa", None, "gx", None),
        P("wa", None, "gx", None),
        P("gx", None),
        P("gx", None),
        P("wa"),
        P("wa"),
        P("wa"),
        P("wa"),
        P("wa", None, None),
        P("wa", None, None),
    )
    return jax.shard_map(
        local,
        mesh=mesh,
        in_specs=placed,
        out_specs=(P("wa", None, "gx", None), P("wa", None, "gx", None), P("gx", None)),
        check_vma=False,
    )
```

```python
import functools

import jax
import jax.numpy as jnp
from jax import lax
from jax.experimental import pallas as pl
from jax.experimental.pallas import tpu as pltpu
from jax.sharding import PartitionSpec as P

floor_share = 0.5
LANES = 128
SUBLANES = 8
HALO = 3
EPS_ROWS = 2
BASE_SUMS = 9
MARK_SUMS = 6
LINE_SUMS = 27
FWD_SUMS = BASE_SUMS + MARK_SUMS
GROUP_LANES = 64
TABLE_COLUMNS = 7
INNER_LIMIT = 6 * 2**20
OUTER_LIMIT = 4 * 2**20
FINISH_LIMIT = 4 * 2**20
VMEM = pl.BlockSpec(memory_space=pltpu.VMEM)
SMEM = pl.BlockSpec(memory_space=pltpu.SMEM)
HBM = pl.BlockSpec(memory_space=pltpu.HBM)


def lane_slice(j):
    return slice(j * LANES, (j + 1) * LANES)


def is_odd(first_row_ref, rows):
    return lax.rem(first_row_ref[0], 2 * rows) != 0


def pack_kernel(first_row_ref, field_hbm, *refs, with_eps):
    if with_eps:
        eps_ref, first_ref, second_ref, stage_ref, sems = refs
    else:
        first_ref, second_ref, stage_ref, sems = refs
    waves, parts, rows, width = field_hbm.shape
    odd = is_odd(first_row_ref, rows)
    chunks = sems.shape[0]
    span = width // chunks
    loads = []
    for n in range(chunks):
        lanes = pl.ds(n * span, span)
        loads.append(
            pltpu.make_async_copy(
                field_hbm.at[:, :, :, lanes], stage_ref.at[:, :, :, lanes], sems.at[n]
            )
        )
        loads[-1].start()
    if with_eps:
        at = HALO * parts * waves
        low = jnp.tile(eps_ref[:EPS_ROWS, :], (SUBLANES // EPS_ROWS, 1))
        high = jnp.tile(eps_ref[rows - EPS_ROWS :, :], (SUBLANES // EPS_ROWS, 1))
        first_ref[at : at + SUBLANES, :] = jnp.where(odd, low, high)
        second_ref[at : at + SUBLANES, :] = jnp.where(odd, high, low)
    for n in range(chunks):
        loads[n].wait()
        for part in range(parts):
            for wave0 in range(0, waves, SUBLANES):
                for lane0 in range(n * span, (n + 1) * span, LANES):
                    lanes = slice(lane0, lane0 + LANES)
                    group = slice(wave0, wave0 + SUBLANES)
                    head = jnp.swapaxes(stage_ref[group, part, :SUBLANES, lanes], 0, 1)
                    tail = jnp.swapaxes(stage_ref[group, part, rows - SUBLANES :, lanes], 0, 1)
                    for k in range(HALO):
                        at = (k * parts + part) * waves + wave0
                        low = head[k]
                        high = tail[SUBLANES - HALO + k]
                        first_ref[at : at + SUBLANES, lanes] = jnp.where(odd, low, high)
                        second_ref[at : at + SUBLANES, lanes] = jnp.where(odd, high, low)


def outer_rows(first_row, field, eps=None):
    waves, parts, rows, width = field.shape
    height = HALO * parts * waves + (0 if eps is None else SUBLANES)
    shape = jax.ShapeDtypeStruct((height, width), jnp.float32)
    return pl.pallas_call(
        functools.partial(pack_kernel, with_eps=eps is not None),
        in_specs=[SMEM, HBM] + ([] if eps is None else [VMEM]),
        out_specs=[VMEM, VMEM],
        out_shape=[shape, shape],
        scratch_shapes=[
            pltpu.VMEM(field.shape, jnp.float32),
            pltpu.SemaphoreType.DMA((8,)),
        ],
        compiler_params=pltpu.CompilerParams(vmem_limit_bytes=INNER_LIMIT),
        name="outer_rows",
    )(first_row, field, *(() if eps is None else (eps,)))


def lane_neighbours(load, count):
    lane = lax.broadcasted_iota(jnp.int32, (SUBLANES, LANES), 1)
    at_low = lane == 0
    at_high = lane == LANES - 1
    zero = jnp.zeros((SUBLANES, LANES), jnp.float32)
    tile = load(0)
    up_before = zero
    down_here = pltpu.roll(tile, LANES - 1, 1)
    for j in range(count):
        up_here = pltpu.roll(tile, 1, 1)
        if j + 1 < count:
            following = load(j + 1)
            down_after = pltpu.roll(following, LANES - 1, 1)
        else:
            following, down_after = None, zero
        yield (
            j,
            tile,
            jnp.where(at_low, up_before, up_here) + jnp.where(at_high, down_after, down_here),
        )
        tile, up_before, down_here = following, up_here, down_after


class Rows:
    def __init__(self, x_ref, z_ref, u_ref, diag_ref, inv_ref, wave_ref):
        self.x, self.z, self.u = x_ref, z_ref, u_ref
        self.diag, self.inv, self.wave = diag_ref, inv_ref, wave_ref
        _, self.parts, self.waves, width = x_ref.shape
        self.rows = x_ref.shape[0] - 2 * HALO
        self.tiles = width // LANES

    def groups(self):
        return [slice(w, w + SUBLANES) for w in range(0, self.waves, SUBLANES)]

    def column(self, index, group):
        return self.wave[index, group, :]

    def set_diagonal(self, i, eps_row):
        for group in self.groups():
            squared_k = self.column(0, group)
            for j in range(self.tiles):
                lanes = lane_slice(j)
                diagonal = 4.0 - squared_k * jnp.broadcast_to(eps_row(lanes), (SUBLANES, LANES))
                self.diag[i, group, lanes] = diagonal
                self.inv[i, group, lanes] = 1.0 / diagonal

    def residual(self, i):
        for group in self.groups():
            both = [
                lane_neighbours(
                    lambda j, part=part: self.x[i + 1, part, group, lane_slice(j)], self.tiles
                )
                for part in range(self.parts)
            ]
            for steps in zip(*both):
                for part, (j, centre, sides) in enumerate(steps):
                    lanes = lane_slice(j)
                    around = self.x[i, part, group, lanes] + self.x[i + 2, part, group, lanes]
                    self.z[i, part, group, lanes] = (
                        around + sides - self.diag[i, group, lanes] * centre
                    ) * self.inv[i, group, lanes]

    def image(self, i):
        for group in self.groups():
            both = [
                lane_neighbours(
                    lambda j, part=part: self.z[i + 1, part, group, lane_slice(j)], self.tiles
                )
                for part in range(self.parts)
            ]
            for steps in zip(*both):
                for part, (j, centre, sides) in enumerate(steps):
                    lanes = lane_slice(j)
                    around = self.z[i, part, group, lanes] + self.z[i + 2, part, group, lanes]
                    image = self.diag[i + 1, group, lanes] * centre - (around + sides)
                    self.u[i, part, group, lanes] = image * self.inv[i + 1, group, lanes]

    def vectors(self, i, group):
        both = [
            lane_neighbours(
                lambda j, part=part: self.u[i + 1, part, group, lane_slice(j)], self.tiles
            )
            for part in range(self.parts)
        ]
        for steps in zip(*both):
            lanes = lane_slice(steps[0][0])
            diagonal = self.diag[i + 2, group, lanes]
            r, v, w = [], [], []
            for part, (_, centre, sides) in enumerate(steps):
                r.append(diagonal * self.z[i + 2, part, group, lanes])
                v.append(diagonal * centre)
                around = self.u[i, part, group, lanes] + self.u[i + 2, part, group, lanes]
                w.append(v[-1] - (around + sides))
            yield steps[0][0], r, v, w

    def twice(self, i, group, sums):
        rr, rv_re, rv_im, vv, wr_re, wr_im, wv_re, wv_im, ww = sums
        for _, r, v, w in self.vectors(i, group):
            rr += r[0] * r[0] + r[1] * r[1]
            rv_re += r[0] * v[0] + r[1] * v[1]
            rv_im += r[0] * v[1] - r[1] * v[0]
            vv += v[0] * v[0] + v[1] * v[1]
            wr_re += w[0] * r[0] + w[1] * r[1]
            wr_im += w[0] * r[1] - w[1] * r[0]
            wv_re += w[0] * v[0] + w[1] * v[1]
            wv_im += w[0] * v[1] - w[1] * v[0]
            ww += w[0] * w[0] + w[1] * w[1]
        return rr, rv_re, rv_im, vv, wr_re, wr_im, wv_re, wv_im, ww

    def any_at(self, table_ref, row):
        hit = table_ref[0] == row
        for w in range(1, self.waves):
            hit = jnp.logical_or(hit, table_ref[w] == row)
        return hit

    def source(self, i, first_row, total_rows, side_row_ref, side_ref):
        row = first_row + i - 2
        row = jnp.where(row < 0, row + total_rows, row)
        row = jnp.where(row >= total_rows, row - total_rows, row)

        @pl.when(self.any_at(side_row_ref, row))
        def _():
            for group in self.groups():
                cosine, sine = self.frame(i - 2, group)
                chosen = self.column(5, group) == row.astype(jnp.float32)
                for j in range(self.tiles):
                    lanes = lane_slice(j)
                    re = side_ref[group, 0, lanes]
                    im = side_ref[group, 1, lanes]
                    inverse = self.inv[i, group, lanes]
                    self.z[i, 0, group, lanes] += jnp.where(
                        chosen, (cosine * re - sine * im) * inverse, 0.0
                    )
                    self.z[i, 1, group, lanes] += jnp.where(
                        chosen, (sine * re + cosine * im) * inverse, 0.0
                    )

    def frame(self, row, group):
        below = row < 0
        above = row >= self.rows
        return (
            jnp.where(below, self.column(1, group), jnp.where(above, self.column(3, group), 1.0)),
            jnp.where(below, self.column(2, group), jnp.where(above, self.column(4, group), 0.0)),
        )


def wave_column(ref, wave0):
    sublane = lax.broadcasted_iota(jnp.int32, (SUBLANES, LANES), 0)
    out = jnp.zeros((SUBLANES, LANES), jnp.float32)
    for k in range(SUBLANES):
        out = jnp.where(sublane == k, ref[wave0 + k].astype(jnp.float32), out)
    return out


def fill_table(table_ref, wave_refs, first_row, rows, total_rows, sign):
    squared_k_ref, cosine_ref, sine_ref, source_ref, monitor_ref = wave_refs
    at_first = first_row == 0
    at_last = first_row == total_rows - rows
    for wave0 in range(0, table_ref.shape[1], SUBLANES):
        group = slice(wave0, wave0 + SUBLANES)
        cosine = wave_column(cosine_ref, wave0)
        sine = sign * wave_column(sine_ref, wave0)
        table_ref[0, group, :] = wave_column(squared_k_ref, wave0)
        table_ref[1, group, :] = jnp.where(at_first, cosine, 1.0)
        table_ref[2, group, :] = jnp.where(at_first, -sine, 0.0)
        table_ref[3, group, :] = jnp.where(at_last, cosine, 1.0)
        table_ref[4, group, :] = jnp.where(at_last, sine, 0.0)
        table_ref[5, group, :] = wave_column(source_ref, wave0)
        table_ref[6, group, :] = wave_column(monitor_ref, wave0)


def lanes_of(out, totals, wave0, offset):
    lane = lax.broadcasted_iota(jnp.int32, (SUBLANES, LANES), 1)
    base = wave0 // SUBLANES * GROUP_LANES + offset
    for n, total in enumerate(totals):
        out = jnp.where(lane == base + n, jnp.sum(total, axis=1, keepdims=True), out)
    return out


def inner_kernel(*refs, forward, total_rows):
    first_row_ref, *wave_refs = refs[:6]
    field_hbm, refs = refs[6], refs[7:]
    side_row_ref = wave_refs[3]
    if forward:
        (eps_ref, side_ref) = refs[:2]
        (x_ref, z_ref, u_ref, sums_ref, diag_ref, inv_ref, stage_ref, table_ref, sems) = refs[2:]
    else:
        (diag_ref, inv_ref) = refs[:2]
        (x_ref, z_ref, u_ref, sums_ref, stage_ref, table_ref, sems) = refs[2:]
    step = Rows(x_ref, z_ref, u_ref, diag_ref, inv_ref, table_ref)
    rows, waves = step.rows, step.waves
    chunks = sems.shape[0]
    span = step.tiles * LANES // chunks
    loads = []
    for n in range(chunks):
        lanes = pl.ds(n * span, span)
        loads.append(
            pltpu.make_async_copy(
                field_hbm.at[:, :, :, lanes], stage_ref.at[:, :, :, lanes], sems.at[n]
            )
        )
        loads[-1].start()
    fill_table(
        table_ref, wave_refs, first_row_ref[0], rows, total_rows, 1.0 if forward else -1.0
    )
    if forward:
        for row in range(rows):
            step.set_diagonal(row + 2, lambda lanes, row=row: eps_ref[row : row + 1, lanes])
    for n in range(chunks):
        loads[n].wait()
        for part in range(step.parts):
            for group in step.groups():
                for row0 in range(0, rows, SUBLANES):
                    for lane0 in range(n * span, (n + 1) * span, LANES):
                        lanes = slice(lane0, lane0 + LANES)
                        x_ref[HALO + row0 : HALO + row0 + SUBLANES, part, group, lanes] = (
                            jnp.swapaxes(
                                stage_ref[group, part, row0 : row0 + SUBLANES, lanes], 0, 1
                            )
                        )

    def residual(i, _):
        step.residual(i)
        if forward:
            step.source(i, first_row_ref[0], total_rows, side_row_ref, side_ref)
        return 0

    def image(i, _):
        step.image(i)
        return 0

    lax.fori_loop(3, rows + 1, residual, 0)
    lax.fori_loop(3, rows - 1, image, 0)
    zero = jnp.zeros((SUBLANES, LANES), jnp.float32)
    out = zero
    for group in step.groups():
        sums = lax.fori_loop(
            3,
            rows - 3,
            lambda i, sums, group=group: step.twice(i, group, sums),
            (zero,) * BASE_SUMS,
        )
        out = lanes_of(out, sums, group.start, 0 if forward else FWD_SUMS)
    sums_ref[...] = out


def outer_kernel(*refs, forward, total_rows):
    first_row_ref, *wave_refs = refs[:6]
    row_ref, mark_row_ref = wave_refs[3:]
    first_ref, second_ref = refs[6:8]
    if forward:
        (part_ref, _, _, _, _, _, side_ref, mark_ref) = refs[8:16]
        (x_ref, z_ref, u_ref, diag_ref, inv_ref, sums_ref, table_ref, mark_sums) = refs[16:]
    else:
        (part_ref, _, _, _, diag_ref, inv_ref, mark_ref, fwd_sums_ref) = refs[8:16]
        (x_ref, z_ref, u_ref, sums_ref, line_ref, table_ref, line_sums, g_ref) = refs[16:]
    step = Rows(x_ref, z_ref, u_ref, diag_ref, inv_ref, table_ref)
    rows, parts, waves, tiles = step.rows, step.parts, step.waves, step.tiles
    odd = is_odd(first_row_ref, rows)
    first_row = first_row_ref[0]
    fill_table(table_ref, wave_refs, first_row, rows, total_rows, 1.0 if forward else -1.0)
    for group in step.groups():
        for base, offset, swap in ((0, 1, False), (HALO + rows, 3, True)):
            cosine = step.column(offset, group)
            sine = step.column(offset + 1, group)
            for k in range(HALO):
                for j in range(tiles):
                    lanes = lane_slice(j)
                    values = []
                    for part in range(parts):
                        at = (k * parts + part) * waves + group.start
                        one = first_ref[at : at + SUBLANES, lanes]
                        two = second_ref[at : at + SUBLANES, lanes]
                        values.append(jnp.where(odd, two, one) if swap else jnp.where(odd, one, two))
                    re, im = values
                    x_ref[base + k, 0, group, lanes] = cosine * re - sine * im
                    x_ref[base + k, 1, group, lanes] = sine * re + cosine * im
    if forward:
        at = HALO * parts * waves
        for k in range(EPS_ROWS):

            def above_eps(lanes, k=k):
                row = slice(at + k, at + k + 1)
                return jnp.where(odd, first_ref[row, lanes], second_ref[row, lanes])

            def below_eps(lanes, k=k):
                row = slice(at + k, at + k + 1)
                return jnp.where(odd, second_ref[row, lanes], first_ref[row, lanes])

            step.set_diagonal(k, above_eps)
            step.set_diagonal(rows + 2 + k, below_eps)

    def outer(t, count):
        return jnp.where(t < 3, t, t + count - 6)

    def residual(t, _):
        i = outer(t, rows + 4)
        step.residual(i)
        if forward:
            step.source(i, first_row, total_rows, row_ref, side_ref)
        return 0

    def image(t, _):
        step.image(outer(t, rows + 2))
        return 0

    lax.fori_loop(0, 6, residual, 0)
    lax.fori_loop(0, 6, image, 0)
    zero = jnp.zeros((SUBLANES, LANES), jnp.float32)
    base_sums = []
    for group in step.groups():
        base_sums.append(
            lax.fori_loop(
                0,
                6,
                lambda t, sums, group=group: step.twice(outer(t, rows), group, sums),
                (zero,) * BASE_SUMS,
            )
        )
    if forward:
        mark_sums[...] = jnp.zeros_like(mark_sums)

        def mark_at(i, _):
            row = first_row + i

            @pl.when(step.any_at(mark_row_ref, row))
            def _():
                for group in step.groups():
                    chosen = step.column(6, group) == row.astype(jnp.float32)
                    for j in range(tiles):
                        lanes = lane_slice(j)
                        m_re = jnp.where(chosen, mark_ref[group, 0, lanes], 0.0)
                        m_im = jnp.where(chosen, mark_ref[group, 1, lanes], 0.0)
                        for n, (ref, shift) in enumerate(((x_ref, 3), (z_ref, 2), (u_ref, 1))):
                            f_re = ref[i + shift, 0, group, lanes]
                            f_im = ref[i + shift, 1, group, lanes]
                            mark_sums[2 * n, group] += m_re * f_re + m_im * f_im
                            mark_sums[2 * n + 1, group] += m_re * f_im - m_im * f_re

            return 0

        lax.fori_loop(0, rows, mark_at, 0)
        extra, count = mark_sums, MARK_SUMS
    else:
        line_terms(step, first_row, total_rows, mark_row_ref, mark_ref, line_ref, line_sums, g_ref)
        extra, count = line_sums, LINE_SUMS
    out = part_ref[...]
    new = jnp.zeros((SUBLANES, LANES), jnp.float32)
    for n, group in enumerate(step.groups()):
        more = list(base_sums[n]) + [extra[k, group] for k in range(count)]
        new = lanes_of(new, more, group.start, 0 if forward else FWD_SUMS)
    out = out + new
    if forward:
        sums_ref[...] = out
    else:
        out = out + fwd_sums_ref[...]
        for n in range(sums_ref.shape[0]):
            sums_ref[n] = out


def distance_to(row, first_row, total_rows):
    away = row - first_row
    away = jnp.where(away >= total_rows - 2, away - total_rows, away)
    return jnp.where(away < -2, away + total_rows, away)


def dot(a, b):
    return a[0] * b[0] + a[1] * b[1], a[0] * b[1] - a[1] * b[0]


def line_terms(step, first_row, total_rows, mark_row_ref, mark_ref, line_ref, line_sums, g_ref):
    rows, tiles = step.rows, step.tiles
    line_ref[...] = jnp.zeros_like(line_ref)
    line_sums[...] = jnp.zeros_like(line_sums)
    sublane = lax.broadcasted_iota(jnp.int32, (SUBLANES, LANES), 0)

    def one_wave(w, _):
        away = distance_to(mark_row_ref[w], first_row, total_rows)

        @pl.when(away <= rows + 1)
        def _():
            group = pl.ds(pl.multiple_of((w // SUBLANES) * SUBLANES, SUBLANES), SUBLANES)
            mine = sublane == w % SUBLANES
            cosine, sine = step.frame(away, group)
            before = jnp.maximum(away + 1, 0)
            after = jnp.minimum(away + 3, rows + 3)
            for j in range(tiles):
                lanes = lane_slice(j)
                m_re = jnp.where(mine, mark_ref[group, 0, lanes], 0.0)
                m_im = jnp.where(mine, mark_ref[group, 1, lanes], 0.0)
                g = (cosine * m_re + sine * m_im, sine * m_re - cosine * m_im)
                inverse = step.inv[away + 2, group, lanes]
                for part in range(2):
                    z = g[part] * inverse
                    g_ref[0, part, :, lanes] = g[part]
                    g_ref[1, part, :, lanes] = z
                    g_ref[2, part, :, lanes] = -z * step.inv[before, group, lanes]
                    g_ref[4, part, :, lanes] = -z * step.inv[after, group, lanes]
            for part in range(2):
                for j, _, sides in lane_neighbours(
                    lambda j, part=part: g_ref[1, part, :, lane_slice(j)], tiles
                ):
                    lanes = lane_slice(j)
                    image = g_ref[0, part, :, lanes] - sides
                    g_ref[5, part, :, lanes] = image
                    g_ref[3, part, :, lanes] = image * step.inv[away + 2, group, lanes]
            for part in range(2):
                for j in range(tiles):
                    lanes = lane_slice(j)
                    for n in range(4):
                        line_ref[n, part, group, lanes] += g_ref[n + 1, part, :, lanes]
            for k in range(-2, 3):

                @pl.when(jnp.logical_and(away + k >= 0, away + k < rows))
                def _(k=k):
                    zero = jnp.zeros((SUBLANES, LANES), jnp.float32)
                    totals = [zero] * LINE_SUMS

                    def add(at, pair):
                        totals[at] = totals[at] + pair[0]
                        totals[at + 1] = totals[at + 1] + pair[1]

                    if abs(k) < 2:
                        sides_of = [
                            [
                                sides
                                for _, _, sides in lane_neighbours(
                                    lambda j, part=part: g_ref[3 + k, part, :, lane_slice(j)],
                                    tiles,
                                )
                            ]
                            for part in range(2)
                        ]
                    for j, r, v, w_vec in step.vectors(away + k, group):
                        lanes = lane_slice(j)
                        get = lambda n: [g_ref[n, part, :, lanes] for part in range(2)]
                        r = [jnp.where(mine, t, 0.0) for t in r]
                        v = [jnp.where(mine, t, 0.0) for t in v]
                        w_vec = [jnp.where(mine, t, 0.0) for t in w_vec]
                        if abs(k) == 2:
                            wg = [-t for t in get(2 if k < 0 else 4)]
                        elif abs(k) == 1:
                            vg = [-t for t in get(1)]
                            mid = get(3)
                            wg = [vg[p] - mid[p] - sides_of[p][j] for p in range(2)]
                        else:
                            g, vg, low, high = get(0), get(5), get(2), get(4)
                            wg = [
                                vg[p] - (low[p] + high[p]) - sides_of[p][j] for p in range(2)
                            ]
                        add(0, dot(wg, r))
                        add(2, dot(wg, v))
                        add(4, dot(w_vec, wg))
                        totals[6] = totals[6] + dot(wg, wg)[0]
                        if abs(k) < 2:
                            add(7, dot(r, vg))
                            add(9, dot(v, vg))
                            add(11, dot(w_vec, vg))
                            add(13, dot(wg, vg))
                            totals[15] = totals[15] + dot(vg, vg)[0]
                        if k == 0:
                            add(16, dot(r, g))
                            add(18, dot(g, v))
                            add(20, dot(g, vg))
                            add(22, dot(w_vec, g))
                            add(24, dot(wg, g))
                            totals[26] = totals[26] + dot(g, g)[0]
                    used = 7 if abs(k) == 2 else 16 if abs(k) == 1 else LINE_SUMS
                    for n in range(used):
                        line_sums[n, group] += totals[n]

        return 0

    lax.fori_loop(0, step.waves, one_wave, 0)


def array(*shape):
    return jax.ShapeDtypeStruct(shape, jnp.float32)


def inner_rows(forward, field, scalars, extra, total_rows):
    waves, parts, rows, width = field.shape
    args = (*scalars, field, *extra)
    out_shape = [
        array(rows + 6, parts, waves, width),
        array(rows + 4, parts, waves, width),
        array(rows + 2, parts, waves, width),
        array(SUBLANES, LANES),
    ]
    if forward:
        out_shape += [array(rows + 4, waves, width)] * 2
    return pl.pallas_call(
        functools.partial(inner_kernel, forward=forward, total_rows=total_rows),
        in_specs=[SMEM] * 6 + [HBM, VMEM, VMEM],
        out_specs=[VMEM] * len(out_shape),
        out_shape=out_shape,
        scratch_shapes=[
            pltpu.VMEM((waves, parts, rows, width), jnp.float32),
            pltpu.VMEM((TABLE_COLUMNS, waves, LANES), jnp.float32),
            pltpu.SemaphoreType.DMA((4,)),
        ],
        compiler_params=pltpu.CompilerParams(vmem_limit_bytes=INNER_LIMIT),
        name="forward_inner" if forward else "adjoint_inner",
    )(*args)


def outer_rows_solve(forward, scalars, received, inner, more, copies, total_rows):
    x, z, u, sums, diag, inv = inner
    waves = x.shape[2]
    args = (*scalars, *received, sums, x, z, u, diag, inv, *more)
    scratch = [pltpu.VMEM((TABLE_COLUMNS, waves, LANES), jnp.float32)]
    if forward:
        out_shape = [array(*a.shape) for a in (x, z, u, diag, inv, sums)]
        aliases = {9: 0, 10: 1, 11: 2, 12: 3, 13: 4}
        scratch += [pltpu.VMEM((MARK_SUMS, waves, LANES), jnp.float32)]
    else:
        out_shape = [array(*a.shape) for a in (x, z, u)] + [
            array(copies, SUBLANES, LANES),
            array(4, 2, waves, x.shape[-1]),
        ]
        aliases = {9: 0, 10: 1, 11: 2}
        scratch += [
            pltpu.VMEM((LINE_SUMS, waves, LANES), jnp.float32),
            pltpu.VMEM((6, 2, SUBLANES, x.shape[-1]), jnp.float32),
        ]
    return pl.pallas_call(
        functools.partial(outer_kernel, forward=forward, total_rows=total_rows),
        in_specs=[SMEM] * 6 + [VMEM] * (len(args) - 6),
        out_specs=[VMEM] * len(out_shape),
        out_shape=out_shape,
        scratch_shapes=scratch,
        input_output_aliases=aliases,
        compiler_params=pltpu.CompilerParams(vmem_limit_bytes=OUTER_LIMIT),
        name="forward_outer" if forward else "adjoint_outer",
    )(*args)


def finish_kernel(
    first_row_ref,
    squared_k_ref,
    mark_row_ref,
    sums_ref,
    xf_ref,
    zf_ref,
    uf_ref,
    xa_ref,
    _z_in,
    _u_in,
    line_ref,
    fwd_hbm,
    adj_hbm,
    grad_ref,
    za_ref,
    ua_ref,
    coef_ref,
    fwd_stage,
    adj_stage,
    sems,
    *,
    total_rows,
):
    waves, parts, rows, width = fwd_hbm.shape
    tiles = width // LANES
    groups = [slice(w, w + SUBLANES) for w in range(0, waves, SUBLANES)]

    def column(index, group):
        return coef_ref[index, group, :]

    sums = jnp.sum(sums_ref[...], axis=0)
    for group in groups:
        base = group.start // SUBLANES * GROUP_LANES
        cols = [
            jnp.broadcast_to(sums[:, base + n : base + n + 1], (SUBLANES, LANES))
            for n in range(FWD_SUMS + BASE_SUMS + LINE_SUMS)
        ]
        fwd_coefs = step_lengths(*cols[:BASE_SUMS])
        a_re, a_im, b_re, b_im = fwd_coefs
        s0_re, s0_im, s1_re, s1_im, s2_re, s2_im = cols[BASE_SUMS:FWD_SUMS]
        over_re = s0_re + (a_re * s1_re - a_im * s1_im) + (b_re * s2_re - b_im * s2_im)
        over_im = s0_im + (a_re * s1_im + a_im * s1_re) + (b_re * s2_im + b_im * s2_re)
        adj_cols = cols[FWD_SUMS:]
        adj_coefs = step_lengths(
            *with_line(adj_cols[:BASE_SUMS], adj_cols[BASE_SUMS:], over_re, -over_im)
        )
        twice_k = 2.0 * wave_column(squared_k_ref, group.start)
        for n, value in enumerate((*fwd_coefs, *adj_coefs, twice_k, over_re, -over_im)):
            coef_ref[n, group, :] = value

    def one_wave(w, _):
        away = distance_to(mark_row_ref[w], first_row_ref[0], total_rows)

        @pl.when(away <= rows)
        def _():
            group = pl.ds(pl.multiple_of((w // SUBLANES) * SUBLANES, SUBLANES), SUBLANES)
            mine = lax.broadcasted_iota(jnp.int32, (SUBLANES, LANES), 0) == w % SUBLANES
            b_re = jnp.where(mine, column(9, group), 0.0)
            b_im = jnp.where(mine, column(10, group), 0.0)
            for n, (ref, shift, k) in enumerate(
                ((za_ref, 2, 0), (ua_ref, 1, -1), (ua_ref, 1, 0), (ua_ref, 1, 1))
            ):

                @pl.when(jnp.logical_and(away + k >= 0, away + k < rows))
                def _(n=n, ref=ref, at=away + k + shift):
                    for j in range(tiles):
                        lanes = lane_slice(j)
                        re = line_ref[n, 0, group, lanes]
                        im = line_ref[n, 1, group, lanes]
                        ref[at, 0, group, lanes] += b_re * re - b_im * im
                        ref[at, 1, group, lanes] += b_re * im + b_im * re

        return 0

    lax.fori_loop(0, waves, one_wave, 0)
    sublane = lax.broadcasted_iota(jnp.int32, (SUBLANES, LANES), 0)

    def copies(j, slot):
        at = pl.ds(j * LANES, LANES)
        if not isinstance(j, int):
            at = pl.ds(pl.multiple_of(j * LANES, LANES), LANES)
        return [
            pltpu.make_async_copy(fwd_stage.at[slot], fwd_hbm.at[:, :, :, at], sems.at[slot, 0]),
            pltpu.make_async_copy(adj_stage.at[slot], adj_hbm.at[:, :, :, at], sems.at[slot, 1]),
        ]

    def tile_step(j, _):
        slot = lax.rem(j, 2)
        lanes = pl.ds(pl.multiple_of(j * LANES, LANES), LANES)

        @pl.when(j >= 2)
        def _():
            for copy in copies(j - 2, slot):
                copy.wait()

        for row0 in range(0, rows, SUBLANES):
            terms = [jnp.zeros((SUBLANES, LANES), jnp.float32)] * SUBLANES
            for group in groups:
                coefs = [column(n, group) for n in range(9)]
                results = [[], [], [], []]
                for k in range(SUBLANES):
                    row = row0 + k
                    values = []
                    for base, x_ref, z_ref, u_ref in (
                        (0, xf_ref, zf_ref, uf_ref),
                        (4, xa_ref, za_ref, ua_ref),
                    ):
                        a_re, a_im, b_re, b_im = coefs[base : base + 4]
                        z_re = z_ref[row + 2, 0, group, lanes]
                        z_im = z_ref[row + 2, 1, group, lanes]
                        u_re = u_ref[row + 1, 0, group, lanes]
                        u_im = u_ref[row + 1, 1, group, lanes]
                        values.append(
                            x_ref[row + HALO, 0, group, lanes]
                            + (a_re * z_re - a_im * z_im)
                            + (b_re * u_re - b_im * u_im)
                        )
                        values.append(
                            x_ref[row + HALO, 1, group, lanes]
                            + (a_re * z_im + a_im * z_re)
                            + (b_re * u_im + b_im * u_re)
                        )
                    f_re, f_im, g_re, g_im = values
                    terms[k] = terms[k] + coefs[8] * (g_re * f_re - g_im * f_im)
                    for n in range(4):
                        results[n].append(values[n])
                for n, (ref, part) in enumerate(
                    ((fwd_stage, 0), (fwd_stage, 1), (adj_stage, 0), (adj_stage, 1))
                ):
                    ref[slot, group, part, row0 : row0 + SUBLANES, :] = jnp.swapaxes(
                        jnp.stack(results[n]), 0, 1
                    )
            out = jnp.zeros((SUBLANES, LANES), jnp.float32)
            for k in range(SUBLANES):
                out = jnp.where(sublane == k, jnp.sum(terms[k], axis=0, keepdims=True), out)
            grad_ref[row0 : row0 + SUBLANES, lanes] = out
        for copy in copies(j, slot):
            copy.start()
        return 0

    lax.fori_loop(0, tiles, tile_step, 0)
    for j in (tiles - 2, tiles - 1):
        for copy in copies(j, j % 2):
            copy.wait()


def finish(scalars, sums, forward_parts, adjoint_parts, line, total_rows):
    x, z, u = forward_parts
    rows, parts, waves, width = x.shape[0] - 2 * HALO, *x.shape[1:]
    field = array(waves, parts, rows, width)
    stage = pltpu.VMEM((2, waves, parts, rows, LANES), jnp.float32)
    return pl.pallas_call(
        functools.partial(finish_kernel, total_rows=total_rows),
        in_specs=[SMEM] * 3 + [VMEM] * 8,
        out_specs=[HBM, HBM, VMEM, VMEM, VMEM],
        out_shape=[field, field, array(rows, width), array(*z.shape), array(*u.shape)],
        scratch_shapes=[
            pltpu.VMEM((11, waves, LANES), jnp.float32),
            stage,
            stage,
            pltpu.SemaphoreType.DMA((2, 2)),
        ],
        input_output_aliases={8: 3, 9: 4},
        compiler_params=pltpu.CompilerParams(vmem_limit_bytes=FINISH_LIMIT),
        name="finish",
    )(*scalars, sums, *forward_parts, *adjoint_parts, line)[:3]


def step_lengths(rr, rv_re, rv_im, vv, wr_re, wr_im, wv_re, wv_im, ww):
    half = floor_share * rr
    bounded = jnp.maximum(rv_re * rv_re + rv_im * rv_im, half * half)
    a_re = rr * rv_re / bounded
    a_im = -rr * rv_im / bounded
    a_sq = a_re * a_re + a_im * a_im
    ts_re = rv_re - a_re * vv - (a_re * wr_re + a_im * wr_im) + a_sq * wv_re
    ts_im = -rv_im - a_im * vv - (a_re * wr_im - a_im * wr_re) + a_sq * wv_im
    tt = vv - 2.0 * (a_re * wv_re + a_im * wv_im) + a_sq * ww
    o_re = ts_re / tt
    o_im = ts_im / tt
    return (a_re + o_re, a_im + o_im, a_im * o_im - a_re * o_re, -(a_re * o_im + a_im * o_re))


def with_line(base, line, b_re, b_im):
    rr, rv_re, rv_im, vv, wr_re, wr_im, wv_re, wv_im, ww = base
    b_sq = b_re * b_re + b_im * b_im

    def pair(at):
        return line[at], line[at + 1]

    def times(p):
        return b_re * p[0] - b_im * p[1], b_re * p[1] + b_im * p[0]

    def times_conj(p):
        return b_re * p[0] + b_im * p[1], b_re * p[1] - b_im * p[0]

    def mixed(re, im, forth, back, both):
        f, h = times(forth), times_conj(back)
        return re + f[0] + h[0] + b_sq * both[0], im + f[1] + h[1] + b_sq * both[1]

    def square(value, cross, both):
        return value + 2.0 * times(cross)[0] + b_sq * both

    rv_re, rv_im = mixed(rv_re, rv_im, pair(7), pair(18), pair(20))
    wr_re, wr_im = mixed(wr_re, wr_im, pair(22), pair(0), pair(24))
    wv_re, wv_im = mixed(wv_re, wv_im, pair(11), pair(2), pair(13))
    rr = square(rr, pair(16), line[26])
    vv = square(vv, pair(9), line[15])
    ww = square(ww, pair(4), line[6])
    return rr, rv_re, rv_im, vv, wr_re, wr_im, wv_re, wv_im, ww


def local(
    warm_field,
    warm_adjoint,
    permittivity,
    design_mask,
    source_row,
    monitor_row,
    wavenumber,
    bloch_phase,
    source_profile,
    monitor_profile,
):
    rows = permittivity.shape[0]
    count = lax.axis_size("gx")
    index = lax.axis_index("gx")
    total_rows = rows * count
    first_row = (index * rows).astype(jnp.int32).reshape(1)
    pairing_one = [(i, i ^ 1) for i in range(count)]
    pairing_two = [(i, (i + 1 if i % 2 else i - 1) % count) for i in range(count)]
    fwd_first, fwd_second = outer_rows(first_row, warm_field, permittivity)
    fwd_got = (
        lax.ppermute(fwd_first, "gx", pairing_one),
        lax.ppermute(fwd_second, "gx", pairing_two),
    )
    adj_first, adj_second = outer_rows(first_row, warm_adjoint)
    adj_got = (
        lax.ppermute(adj_first, "gx", pairing_one),
        lax.ppermute(adj_second, "gx", pairing_two),
    )
    scalars = (
        first_row,
        wavenumber,
        jnp.cos(bloch_phase),
        jnp.sin(bloch_phase),
        source_row,
        monitor_row,
    )
    fx, fz, fu, f_sums, diag, inv = inner_rows(
        True, warm_field, scalars, (permittivity, source_profile), total_rows
    )
    ax, az, au, a_sums = inner_rows(False, warm_adjoint, scalars, (diag, inv), total_rows)
    fx, fz, fu, diag, inv, f_sums = outer_rows_solve(
        True,
        scalars,
        fwd_got,
        (fx, fz, fu, f_sums, diag, inv),
        (source_profile, monitor_profile),
        count,
        total_rows,
    )
    ax, az, au, sums, line = outer_rows_solve(
        False,
        scalars,
        adj_got,
        (ax, az, au, a_sums, diag, inv),
        (monitor_profile, f_sums),
        count,
        total_rows,
    )
    forward, adjoint, partial = finish(
        (first_row, wavenumber, monitor_row),
        lax.all_to_all(sums, "gx", 0, 0, tiled=True),
        (fx, fz, fu),
        (ax, az, au),
        line,
        total_rows,
    )
    summed_terms = lax.all_gather(partial, "wa").sum(axis=0)
    gradient = design_mask.astype(jnp.float32) * summed_terms
    return (forward, adjoint, gradient)


def solution(mesh):
    placed = (
        P("wa", None, "gx", None),
        P("wa", None, "gx", None),
        P("gx", None),
        P("gx", None),
        P("wa"),
        P("wa"),
        P("wa"),
        P("wa"),
        P("wa", None, None),
        P("wa", None, None),
    )
    return jax.shard_map(
        local,
        mesh=mesh,
        in_specs=placed,
        out_specs=(P("wa", None, "gx", None), P("wa", None, "gx", None), P("gx", None)),
        check_vma=False,
    )
```

```python
import functools

import jax
import jax.numpy as jnp
from jax import lax
from jax.experimental import pallas as pl
from jax.experimental.pallas import tpu as pltpu
from jax.sharding import PartitionSpec as P

floor_share = 0.5
LANES = 128
SUBLANES = 8
HALO = 3
EPS_ROWS = 2
BASE_SUMS = 9
MARK_SUMS = 6
LINE_SUMS = 27
FWD_SUMS = BASE_SUMS + MARK_SUMS
GROUP_LANES = 64
TABLE_COLUMNS = 7
INNER_LIMIT = 2 * 2**20
OUTER_LIMIT = 4 * 2**20
FINISH_LIMIT = 10 * 2**20
VMEM = pl.BlockSpec(memory_space=pltpu.VMEM)
SMEM = pl.BlockSpec(memory_space=pltpu.SMEM)
HBM = pl.BlockSpec(memory_space=pltpu.HBM)


def lane_slice(j):
    return slice(j * LANES, (j + 1) * LANES)


def is_odd(first_row_ref, rows):
    return lax.rem(first_row_ref[0], 2 * rows) != 0


def pack_kernel(first_row_ref, field_ref, *refs, with_eps):
    if with_eps:
        eps_ref, first_ref, second_ref = refs
    else:
        first_ref, second_ref = refs
    waves, parts, rows, width = field_ref.shape
    odd = is_odd(first_row_ref, rows)
    pieces = [
        (slice(wave0, wave0 + SUBLANES), part)
        for wave0 in range(0, waves, SUBLANES)
        for part in range(parts)
    ]
    if with_eps:
        at = HALO * parts * waves
        low = jnp.tile(eps_ref[:EPS_ROWS, :], (SUBLANES // EPS_ROWS, 1))
        high = jnp.tile(eps_ref[rows - EPS_ROWS :, :], (SUBLANES // EPS_ROWS, 1))
        first_ref[at : at + SUBLANES, :] = jnp.where(odd, low, high)
        second_ref[at : at + SUBLANES, :] = jnp.where(odd, high, low)
    for group, part in pieces:
        for lane0 in range(0, width, LANES):
            lanes = slice(lane0, lane0 + LANES)
            head = jnp.swapaxes(field_ref[group, part, :SUBLANES, lanes], 0, 1)
            tail = jnp.swapaxes(field_ref[group, part, rows - SUBLANES :, lanes], 0, 1)
            for k in range(HALO):
                at = (k * parts + part) * waves + group.start
                low = head[k]
                high = tail[SUBLANES - HALO + k]
                first_ref[at : at + SUBLANES, lanes] = jnp.where(odd, low, high)
                second_ref[at : at + SUBLANES, lanes] = jnp.where(odd, high, low)


def outer_rows(first_row, field, eps=None):
    waves, parts, rows, width = field.shape
    height = HALO * parts * waves + (0 if eps is None else SUBLANES)
    shape = jax.ShapeDtypeStruct((height, width), jnp.float32)
    return pl.pallas_call(
        functools.partial(pack_kernel, with_eps=eps is not None),
        in_specs=[SMEM, VMEM] + ([] if eps is None else [VMEM]),
        out_specs=[VMEM, VMEM],
        out_shape=[shape, shape],
        compiler_params=pltpu.CompilerParams(
            vmem_limit_bytes=INNER_LIMIT
        ),
        name="outer_rows",
    )(first_row, field, *(() if eps is None else (eps,)))


def lane_neighbours(load, count):
    lane = lax.broadcasted_iota(jnp.int32, (SUBLANES, LANES), 1)
    at_low = lane == 0
    at_high = lane == LANES - 1
    zero = jnp.zeros((SUBLANES, LANES), jnp.float32)
    tile = load(0)
    up_before = zero
    down_here = pltpu.roll(tile, LANES - 1, 1)
    for j in range(count):
        up_here = pltpu.roll(tile, 1, 1)
        if j + 1 < count:
            following = load(j + 1)
            down_after = pltpu.roll(following, LANES - 1, 1)
        else:
            following, down_after = None, zero
        yield (
            j,
            tile,
            jnp.where(at_low, up_before, up_here) + jnp.where(at_high, down_after, down_here),
        )
        tile, up_before, down_here = following, up_here, down_after


class Scalars:
    def __init__(self, whole_ref, real_ref):
        self.whole, self.real = whole_ref, real_ref
        self.waves = real_ref.shape[0] // 3
        self.first_row = whole_ref[0]

    def source(self, w):
        return self.whole[1 + w]

    def monitor(self, w):
        return self.whole[1 + self.waves + w]

    def squared_k(self, w):
        return self.real[w]

    def cosine(self, w):
        return self.real[self.waves + w]

    def sine(self, w):
        return self.real[2 * self.waves + w]


class Rows:
    def __init__(self, x_ref, z_ref, u_ref, diag_ref, inv_ref, wave_ref):
        self.x, self.z, self.u = x_ref, z_ref, u_ref
        self.diag, self.inv, self.wave = diag_ref, inv_ref, wave_ref
        _, self.parts, self.waves, width = x_ref.shape
        self.rows = x_ref.shape[0] - 2 * HALO
        self.tiles = width // LANES

    def groups(self):
        return [slice(w, w + SUBLANES) for w in range(0, self.waves, SUBLANES)]

    def column(self, index, group):
        return self.wave[index, group, :]

    def set_diagonal(self, i, eps_row):
        for group in self.groups():
            squared_k = self.column(0, group)
            for j in range(self.tiles):
                lanes = lane_slice(j)
                diagonal = 4.0 - squared_k * jnp.broadcast_to(eps_row(lanes), (SUBLANES, LANES))
                self.diag[i, group, lanes] = diagonal
                self.inv[i, group, lanes] = 1.0 / diagonal

    def tiles_of(self, ref, i, count, group):
        chains = [
            [
                lane_neighbours(
                    lambda j, at=i + k, part=part: ref[at, part, group, lane_slice(j)], self.tiles
                )
                for part in range(self.parts)
            ]
            for k in range(count)
        ]
        for j in range(self.tiles):
            lanes = lane_slice(j)
            now = [[next(chain)[1:] for chain in row] for row in chains]
            out = []
            for k in range(count):
                row = []
                for part in range(self.parts):
                    low = now[k - 1][part][0] if k else ref[i - 1, part, group, lanes]
                    high = now[k + 1][part][0] if k + 1 < count else ref[i + count, part, group, lanes]
                    centre, sides = now[k][part]
                    row.append((centre, low + high, sides))
                out.append(row)
            yield j, out

    def residual(self, i, count):
        for group in self.groups():
            for j, block in self.tiles_of(self.x, i + 1, count, group):
                lanes = lane_slice(j)
                for k in range(count):
                    diagonal = self.diag[i + k, group, lanes]
                    inverse = self.inv[i + k, group, lanes]
                    for part, (centre, around, sides) in enumerate(block[k]):
                        self.z[i + k, part, group, lanes] = (
                            around + sides - diagonal * centre
                        ) * inverse

    def image(self, i, count):
        for group in self.groups():
            for j, block in self.tiles_of(self.z, i + 1, count, group):
                lanes = lane_slice(j)
                for k in range(count):
                    inverse = self.inv[i + 1 + k, group, lanes]
                    for part, (centre, around, sides) in enumerate(block[k]):
                        self.u[i + k, part, group, lanes] = centre - (around + sides) * inverse

    def vectors(self, i, group, count=1):
        for j, block in self.tiles_of(self.u, i + 1, count, group):
            lanes = lane_slice(j)
            for k in range(count):
                diagonal = self.diag[i + 2 + k, group, lanes]
                r, v, w = [], [], []
                for part, (centre, around, sides) in enumerate(block[k]):
                    r.append(diagonal * self.z[i + 2 + k, part, group, lanes])
                    v.append(diagonal * centre)
                    w.append(v[-1] - (around + sides))
                yield j, r, v, w

    def twice(self, i, group, sums, count):
        rr, rv_re, rv_im, vv, wr_re, wr_im, wv_re, wv_im, ww = sums
        for _, r, v, w in self.vectors(i, group, count):
            rr += r[0] * r[0] + r[1] * r[1]
            rv_re += r[0] * v[0] + r[1] * v[1]
            rv_im += r[0] * v[1] - r[1] * v[0]
            vv += v[0] * v[0] + v[1] * v[1]
            wr_re += w[0] * r[0] + w[1] * r[1]
            wr_im += w[0] * r[1] - w[1] * r[0]
            wv_re += w[0] * v[0] + w[1] * v[1]
            wv_im += w[0] * v[1] - w[1] * v[0]
            ww += w[0] * w[0] + w[1] * w[1]
        return rr, rv_re, rv_im, vv, wr_re, wr_im, wv_re, wv_im, ww

    def any_at(self, row_of, row):
        hit = row_of(0) == row
        for w in range(1, self.waves):
            hit = jnp.logical_or(hit, row_of(w) == row)
        return hit

    def source(self, i, scalars, total_rows, side_ref):
        row = scalars.first_row + i - 2
        row = jnp.where(row < 0, row + total_rows, row)
        row = jnp.where(row >= total_rows, row - total_rows, row)

        @pl.when(self.any_at(scalars.source, row))
        def _():
            for group in self.groups():
                cosine, sine = self.frame(i - 2, group)
                chosen = self.column(5, group) == row.astype(jnp.float32)
                for j in range(self.tiles):
                    lanes = lane_slice(j)
                    re = side_ref[group, 0, lanes]
                    im = side_ref[group, 1, lanes]
                    inverse = self.inv[i, group, lanes]
                    self.z[i, 0, group, lanes] += jnp.where(
                        chosen, (cosine * re - sine * im) * inverse, 0.0
                    )
                    self.z[i, 1, group, lanes] += jnp.where(
                        chosen, (sine * re + cosine * im) * inverse, 0.0
                    )

    def frame(self, row, group):
        below = row < 0
        above = row >= self.rows
        return (
            jnp.where(below, self.column(1, group), jnp.where(above, self.column(3, group), 1.0)),
            jnp.where(below, self.column(2, group), jnp.where(above, self.column(4, group), 0.0)),
        )


def wave_column(value_of, wave0):
    sublane = lax.broadcasted_iota(jnp.int32, (SUBLANES, LANES), 0)
    out = jnp.zeros((SUBLANES, LANES), jnp.float32)
    for k in range(SUBLANES):
        out = jnp.where(sublane == k, value_of(wave0 + k).astype(jnp.float32), out)
    return out


def fill_table(table_ref, scalars, rows, total_rows, sign):
    at_first = scalars.first_row == 0
    at_last = scalars.first_row == total_rows - rows
    for wave0 in range(0, table_ref.shape[1], SUBLANES):
        group = slice(wave0, wave0 + SUBLANES)
        cosine = wave_column(scalars.cosine, wave0)
        sine = sign * wave_column(scalars.sine, wave0)
        table_ref[0, group, :] = wave_column(scalars.squared_k, wave0)
        table_ref[1, group, :] = jnp.where(at_first, cosine, 1.0)
        table_ref[2, group, :] = jnp.where(at_first, -sine, 0.0)
        table_ref[3, group, :] = jnp.where(at_last, cosine, 1.0)
        table_ref[4, group, :] = jnp.where(at_last, sine, 0.0)
        table_ref[5, group, :] = wave_column(scalars.source, wave0)
        table_ref[6, group, :] = wave_column(scalars.monitor, wave0)


def lanes_of(out, totals, wave0, offset):
    lane = lax.broadcasted_iota(jnp.int32, (SUBLANES, LANES), 1)
    base = wave0 // SUBLANES * GROUP_LANES + offset
    for n, total in enumerate(totals):
        out = jnp.where(lane == base + n, jnp.sum(total, axis=1, keepdims=True), out)
    return out


def inner_kernel(*refs, forward, total_rows):
    scalars = Scalars(*refs[:2])
    field_ref, refs = refs[2], refs[3:]
    if forward:
        (eps_ref, side_ref) = refs[:2]
        (x_ref, z_ref, u_ref, sums_ref, diag_ref, inv_ref, table_ref) = refs[2:]
    else:
        (diag_ref, inv_ref) = refs[:2]
        (x_ref, z_ref, u_ref, sums_ref, table_ref) = refs[2:]
    step = Rows(x_ref, z_ref, u_ref, diag_ref, inv_ref, table_ref)
    rows, waves = step.rows, step.waves
    fill_table(table_ref, scalars, rows, total_rows, 1.0 if forward else -1.0)
    if forward:
        for row in range(rows):
            step.set_diagonal(row + 2, lambda lanes, row=row: eps_ref[row : row + 1, lanes])
    def turn(j, _):
        lanes = pl.ds(pl.multiple_of(j * LANES, LANES), LANES)
        for part in range(step.parts):
            for group in step.groups():
                for row0 in range(0, rows, SUBLANES):
                    x_ref[HALO + row0 : HALO + row0 + SUBLANES, part, group, lanes] = (
                        jnp.swapaxes(
                            field_ref[group, part, row0 : row0 + SUBLANES, lanes], 0, 1
                        )
                    )
        return 0

    lax.fori_loop(0, step.tiles, turn, 0)

    def residual(t, _):
        i = 3 + 2 * t
        step.residual(i, 2)
        if forward:
            step.source(i, scalars, total_rows, side_ref)
            step.source(i + 1, scalars, total_rows, side_ref)
        return 0

    def image(t, _):
        step.image(3 + 3 * t, 3)
        return 0

    lax.fori_loop(0, (rows - 2) // 2, residual, 0)
    lax.fori_loop(0, (rows - 4) // 3, image, 0)
    zero = jnp.zeros((SUBLANES, LANES), jnp.float32)
    out = zero
    for group in step.groups():
        sums = lax.fori_loop(
            0,
            (rows - 6) // 2,
            lambda t, sums, group=group: step.twice(3 + 2 * t, group, sums, 2),
            (zero,) * BASE_SUMS,
        )
        out = lanes_of(out, sums, group.start, 0 if forward else FWD_SUMS)
    sums_ref[...] = out


def outer_kernel(*refs, forward, total_rows):
    scalars = Scalars(*refs[:2])
    first_ref, second_ref, refs = refs[2], refs[3], refs[4:]
    if forward:
        (part_ref, _, _, _, _, _, side_ref, mark_ref) = refs[:8]
        (x_ref, z_ref, u_ref, diag_ref, inv_ref, sums_ref, table_ref, mark_sums) = refs[8:]
    else:
        (part_ref, _, _, _, diag_ref, inv_ref, mark_ref, fwd_sums_ref) = refs[:8]
        (x_ref, z_ref, u_ref, sums_ref, line_ref, table_ref, line_sums, g_ref) = refs[8:]
    step = Rows(x_ref, z_ref, u_ref, diag_ref, inv_ref, table_ref)
    rows, parts, waves, tiles = step.rows, step.parts, step.waves, step.tiles
    first_row = scalars.first_row
    odd = lax.rem(first_row, 2 * rows) != 0
    fill_table(table_ref, scalars, rows, total_rows, 1.0 if forward else -1.0)
    for group in step.groups():
        for base, offset, swap in ((0, 1, False), (HALO + rows, 3, True)):
            cosine = step.column(offset, group)
            sine = step.column(offset + 1, group)
            for k in range(HALO):
                for j in range(tiles):
                    lanes = lane_slice(j)
                    values = []
                    for part in range(parts):
                        at = (k * parts + part) * waves + group.start
                        one = first_ref[at : at + SUBLANES, lanes]
                        two = second_ref[at : at + SUBLANES, lanes]
                        values.append(jnp.where(odd, two, one) if swap else jnp.where(odd, one, two))
                    re, im = values
                    x_ref[base + k, 0, group, lanes] = cosine * re - sine * im
                    x_ref[base + k, 1, group, lanes] = sine * re + cosine * im
    if forward:
        at = HALO * parts * waves
        for k in range(EPS_ROWS):

            def above_eps(lanes, k=k):
                row = slice(at + k, at + k + 1)
                return jnp.where(odd, first_ref[row, lanes], second_ref[row, lanes])

            def below_eps(lanes, k=k):
                row = slice(at + k, at + k + 1)
                return jnp.where(odd, second_ref[row, lanes], first_ref[row, lanes])

            step.set_diagonal(k, above_eps)
            step.set_diagonal(rows + 2 + k, below_eps)

    def residual(t, _):
        i = t * (rows + 1)
        step.residual(i, 3)
        if forward:
            for k in range(3):
                step.source(i + k, scalars, total_rows, side_ref)
        return 0

    def image(t, _):
        step.image(t * (rows - 1), 3)
        return 0

    lax.fori_loop(0, 2, residual, 0)
    lax.fori_loop(0, 2, image, 0)
    zero = jnp.zeros((SUBLANES, LANES), jnp.float32)
    base_sums = []
    for group in step.groups():
        base_sums.append(
            lax.fori_loop(
                0,
                2,
                lambda t, sums, group=group: step.twice(t * (rows - 3), group, sums, 3),
                (zero,) * BASE_SUMS,
            )
        )
    if forward:
        mark_sums[...] = jnp.zeros_like(mark_sums)

        def mark_at(i, _):
            row = first_row + i

            @pl.when(step.any_at(scalars.monitor, row))
            def _():
                for group in step.groups():
                    chosen = step.column(6, group) == row.astype(jnp.float32)
                    for j in range(tiles):
                        lanes = lane_slice(j)
                        m_re = jnp.where(chosen, mark_ref[group, 0, lanes], 0.0)
                        m_im = jnp.where(chosen, mark_ref[group, 1, lanes], 0.0)
                        for n, (ref, shift) in enumerate(((x_ref, 3), (z_ref, 2), (u_ref, 1))):
                            f_re = ref[i + shift, 0, group, lanes]
                            f_im = ref[i + shift, 1, group, lanes]
                            mark_sums[2 * n, group] += m_re * f_re + m_im * f_im
                            mark_sums[2 * n + 1, group] += m_re * f_im - m_im * f_re

            return 0

        lax.fori_loop(0, rows, mark_at, 0)
        extra, count = mark_sums, MARK_SUMS
    else:
        line_terms(step, scalars, total_rows, mark_ref, line_ref, line_sums, g_ref)
        extra, count = line_sums, LINE_SUMS
    out = part_ref[...]
    new = jnp.zeros((SUBLANES, LANES), jnp.float32)
    for n, group in enumerate(step.groups()):
        more = list(base_sums[n]) + [extra[k, group] for k in range(count)]
        new = lanes_of(new, more, group.start, 0 if forward else FWD_SUMS)
    out = out + new
    if forward:
        sums_ref[...] = out
    else:
        out = out + fwd_sums_ref[...]
        for n in range(sums_ref.shape[0]):
            sums_ref[n] = out


def distance_to(row, first_row, total_rows):
    away = row - first_row
    away = jnp.where(away >= total_rows - 2, away - total_rows, away)
    return jnp.where(away < -2, away + total_rows, away)


def dot(a, b):
    return a[0] * b[0] + a[1] * b[1], a[0] * b[1] - a[1] * b[0]


def line_terms(step, scalars, total_rows, mark_ref, line_ref, line_sums, g_ref):
    rows, tiles = step.rows, step.tiles
    line_ref[...] = jnp.zeros_like(line_ref)
    line_sums[...] = jnp.zeros_like(line_sums)
    sublane = lax.broadcasted_iota(jnp.int32, (SUBLANES, LANES), 0)

    def one_wave(w, _):
        away = distance_to(scalars.monitor(w), scalars.first_row, total_rows)

        @pl.when(away <= rows + 1)
        def _():
            group = pl.ds(pl.multiple_of((w // SUBLANES) * SUBLANES, SUBLANES), SUBLANES)
            mine = sublane == w % SUBLANES
            cosine, sine = step.frame(away, group)
            before = jnp.maximum(away + 1, 0)
            after = jnp.minimum(away + 3, rows + 3)
            for j in range(tiles):
                lanes = lane_slice(j)
                m_re = jnp.where(mine, mark_ref[group, 0, lanes], 0.0)
                m_im = jnp.where(mine, mark_ref[group, 1, lanes], 0.0)
                g = (cosine * m_re + sine * m_im, sine * m_re - cosine * m_im)
                inverse = step.inv[away + 2, group, lanes]
                for part in range(2):
                    z = g[part] * inverse
                    g_ref[0, part, :, lanes] = g[part]
                    g_ref[1, part, :, lanes] = z
                    g_ref[2, part, :, lanes] = -z * step.inv[before, group, lanes]
                    g_ref[4, part, :, lanes] = -z * step.inv[after, group, lanes]
            for part in range(2):
                for j, _, sides in lane_neighbours(
                    lambda j, part=part: g_ref[1, part, :, lane_slice(j)], tiles
                ):
                    lanes = lane_slice(j)
                    image = g_ref[0, part, :, lanes] - sides
                    g_ref[5, part, :, lanes] = image
                    g_ref[3, part, :, lanes] = image * step.inv[away + 2, group, lanes]
            for part in range(2):
                for j in range(tiles):
                    lanes = lane_slice(j)
                    for n in range(4):
                        line_ref[n, part, group, lanes] += g_ref[n + 1, part, :, lanes]
            for k in range(-2, 3):

                @pl.when(jnp.logical_and(away + k >= 0, away + k < rows))
                def _(k=k):
                    zero = jnp.zeros((SUBLANES, LANES), jnp.float32)
                    totals = [zero] * LINE_SUMS

                    def add(at, pair):
                        totals[at] = totals[at] + pair[0]
                        totals[at + 1] = totals[at + 1] + pair[1]

                    if abs(k) < 2:
                        sides_of = [
                            [
                                sides
                                for _, _, sides in lane_neighbours(
                                    lambda j, part=part: g_ref[3 + k, part, :, lane_slice(j)],
                                    tiles,
                                )
                            ]
                            for part in range(2)
                        ]
                    for j, r, v, w_vec in step.vectors(away + k, group):
                        lanes = lane_slice(j)
                        get = lambda n: [g_ref[n, part, :, lanes] for part in range(2)]
                        r = [jnp.where(mine, t, 0.0) for t in r]
                        v = [jnp.where(mine, t, 0.0) for t in v]
                        w_vec = [jnp.where(mine, t, 0.0) for t in w_vec]
                        if abs(k) == 2:
                            wg = [-t for t in get(2 if k < 0 else 4)]
                        elif abs(k) == 1:
                            vg = [-t for t in get(1)]
                            mid = get(3)
                            wg = [vg[p] - mid[p] - sides_of[p][j] for p in range(2)]
                        else:
                            g, vg, low, high = get(0), get(5), get(2), get(4)
                            wg = [
                                vg[p] - (low[p] + high[p]) - sides_of[p][j] for p in range(2)
                            ]
                        add(0, dot(wg, r))
                        add(2, dot(wg, v))
                        add(4, dot(w_vec, wg))
                        totals[6] = totals[6] + dot(wg, wg)[0]
                        if abs(k) < 2:
                            add(7, dot(r, vg))
                            add(9, dot(v, vg))
                            add(11, dot(w_vec, vg))
                            add(13, dot(wg, vg))
                            totals[15] = totals[15] + dot(vg, vg)[0]
                        if k == 0:
                            add(16, dot(r, g))
                            add(18, dot(g, v))
                            add(20, dot(g, vg))
                            add(22, dot(w_vec, g))
                            add(24, dot(wg, g))
                            totals[26] = totals[26] + dot(g, g)[0]
                    used = 7 if abs(k) == 2 else 16 if abs(k) == 1 else LINE_SUMS
                    for n in range(used):
                        line_sums[n, group] += totals[n]

        return 0

    lax.fori_loop(0, step.waves, one_wave, 0)


def array(*shape):
    return jax.ShapeDtypeStruct(shape, jnp.float32)


def inner_rows(forward, field, scalars, extra, total_rows):
    waves, parts, rows, width = field.shape
    args = (*scalars, field, *extra)
    out_shape = [
        array(rows + 6, parts, waves, width),
        array(rows + 4, parts, waves, width),
        array(rows + 2, parts, waves, width),
        array(SUBLANES, LANES),
    ]
    if forward:
        out_shape += [array(rows + 4, waves, width)] * 2
    return pl.pallas_call(
        functools.partial(inner_kernel, forward=forward, total_rows=total_rows),
        in_specs=[SMEM] * 2 + [VMEM, VMEM, VMEM],
        out_specs=[VMEM] * len(out_shape),
        out_shape=out_shape,
        scratch_shapes=[
            pltpu.VMEM((TABLE_COLUMNS, waves, LANES), jnp.float32),
        ],
        compiler_params=pltpu.CompilerParams(
            vmem_limit_bytes=INNER_LIMIT
        ),
        name="forward_inner" if forward else "adjoint_inner",
    )(*args)


def outer_rows_solve(forward, scalars, received, inner, more, copies, total_rows):
    x, z, u, sums, diag, inv = inner
    waves = x.shape[2]
    args = (*scalars, *received, sums, x, z, u, diag, inv, *more)
    scratch = [pltpu.VMEM((TABLE_COLUMNS, waves, LANES), jnp.float32)]
    if forward:
        out_shape = [array(*a.shape) for a in (x, z, u, diag, inv, sums)]
        aliases = {5: 0, 6: 1, 7: 2, 8: 3, 9: 4}
        scratch += [pltpu.VMEM((MARK_SUMS, waves, LANES), jnp.float32)]
    else:
        out_shape = [array(*a.shape) for a in (x, z, u)] + [
            array(copies, SUBLANES, LANES),
            array(4, 2, waves, x.shape[-1]),
        ]
        aliases = {5: 0, 6: 1, 7: 2}
        scratch += [
            pltpu.VMEM((LINE_SUMS, waves, LANES), jnp.float32),
            pltpu.VMEM((6, 2, SUBLANES, x.shape[-1]), jnp.float32),
        ]
    return pl.pallas_call(
        functools.partial(outer_kernel, forward=forward, total_rows=total_rows),
        in_specs=[SMEM] * 2 + [VMEM] * (len(args) - 2),
        out_specs=[VMEM] * len(out_shape),
        out_shape=out_shape,
        scratch_shapes=scratch,
        input_output_aliases=aliases,
        compiler_params=pltpu.CompilerParams(vmem_limit_bytes=OUTER_LIMIT),
        name="forward_outer" if forward else "adjoint_outer",
    )(*args)


def finish_kernel(
    whole_ref,
    real_ref,
    sums_ref,
    xf_ref,
    zf_ref,
    uf_ref,
    xa_ref,
    _z_in,
    _u_in,
    line_ref,
    fwd_hbm,
    adj_hbm,
    grad_ref,
    za_ref,
    ua_ref,
    coef_ref,
    fwd_stage,
    adj_stage,
    sems,
    *,
    total_rows,
):
    waves, parts, rows, width = fwd_hbm.shape
    tiles = width // LANES
    groups = [slice(w, w + SUBLANES) for w in range(0, waves, SUBLANES)]
    scalars = Scalars(whole_ref, real_ref)

    def column(index, group):
        return coef_ref[index, group, :]

    sums = jnp.sum(sums_ref[...], axis=0)
    for group in groups:
        base = group.start // SUBLANES * GROUP_LANES
        cols = [
            jnp.broadcast_to(sums[:, base + n : base + n + 1], (SUBLANES, LANES))
            for n in range(FWD_SUMS + BASE_SUMS + LINE_SUMS)
        ]
        fwd_coefs = step_lengths(*cols[:BASE_SUMS])
        a_re, a_im, b_re, b_im = fwd_coefs
        s0_re, s0_im, s1_re, s1_im, s2_re, s2_im = cols[BASE_SUMS:FWD_SUMS]
        over_re = s0_re + (a_re * s1_re - a_im * s1_im) + (b_re * s2_re - b_im * s2_im)
        over_im = s0_im + (a_re * s1_im + a_im * s1_re) + (b_re * s2_im + b_im * s2_re)
        adj_cols = cols[FWD_SUMS:]
        adj_coefs = step_lengths(
            *with_line(adj_cols[:BASE_SUMS], adj_cols[BASE_SUMS:], over_re, -over_im)
        )
        twice_k = 2.0 * wave_column(scalars.squared_k, group.start)
        for n, value in enumerate((*fwd_coefs, *adj_coefs, twice_k, over_re, -over_im)):
            coef_ref[n, group, :] = value

    def one_wave(w, _):
        away = distance_to(scalars.monitor(w), scalars.first_row, total_rows)

        @pl.when(away <= rows)
        def _():
            group = pl.ds(pl.multiple_of((w // SUBLANES) * SUBLANES, SUBLANES), SUBLANES)
            mine = lax.broadcasted_iota(jnp.int32, (SUBLANES, LANES), 0) == w % SUBLANES
            b_re = jnp.where(mine, column(9, group), 0.0)
            b_im = jnp.where(mine, column(10, group), 0.0)
            for n, (ref, shift, k) in enumerate(
                ((za_ref, 2, 0), (ua_ref, 1, -1), (ua_ref, 1, 0), (ua_ref, 1, 1))
            ):

                @pl.when(jnp.logical_and(away + k >= 0, away + k < rows))
                def _(n=n, ref=ref, at=away + k + shift):
                    for j in range(tiles):
                        lanes = lane_slice(j)
                        re = line_ref[n, 0, group, lanes]
                        im = line_ref[n, 1, group, lanes]
                        ref[at, 0, group, lanes] += b_re * re - b_im * im
                        ref[at, 1, group, lanes] += b_re * im + b_im * re

        return 0

    lax.fori_loop(0, waves, one_wave, 0)
    sublane = lax.broadcasted_iota(jnp.int32, (SUBLANES, LANES), 0)

    copies = []
    for row0 in range(0, rows, SUBLANES):
        for group in groups:

            def tile_step(j, row0=row0, group=group):
                lanes = pl.ds(pl.multiple_of(j * LANES, LANES), LANES)
                coefs = [column(n, group) for n in range(9)]
                results = [[], [], [], []]
                out = jnp.zeros((SUBLANES, LANES), jnp.float32)
                for k in range(SUBLANES):
                    row = row0 + k
                    values = []
                    for base, x_ref, z_ref, u_ref in (
                        (0, xf_ref, zf_ref, uf_ref),
                        (4, xa_ref, za_ref, ua_ref),
                    ):
                        a_re, a_im, b_re, b_im = coefs[base : base + 4]
                        z_re = z_ref[row + 2, 0, group, lanes]
                        z_im = z_ref[row + 2, 1, group, lanes]
                        u_re = u_ref[row + 1, 0, group, lanes]
                        u_im = u_ref[row + 1, 1, group, lanes]
                        values.append(
                            x_ref[row + HALO, 0, group, lanes]
                            + (a_re * z_re - a_im * z_im)
                            + (b_re * u_re - b_im * u_im)
                        )
                        values.append(
                            x_ref[row + HALO, 1, group, lanes]
                            + (a_re * z_im + a_im * z_re)
                            + (b_re * u_im + b_im * u_re)
                        )
                    f_re, f_im, g_re, g_im = values
                    term = coefs[8] * (g_re * f_re - g_im * f_im)
                    out = jnp.where(sublane == k, jnp.sum(term, axis=0, keepdims=True), out)
                    for n in range(4):
                        results[n].append(values[n])
                for n, (ref, part) in enumerate(
                    ((fwd_stage, 0), (fwd_stage, 1), (adj_stage, 0), (adj_stage, 1))
                ):
                    ref[group, part, row0 : row0 + SUBLANES, lanes] = jnp.swapaxes(
                        jnp.stack(results[n]), 0, 1
                    )
                if group.start:
                    out = out + grad_ref[row0 : row0 + SUBLANES, lanes]
                grad_ref[row0 : row0 + SUBLANES, lanes] = out

            def two_tiles(t, _, tile_step=tile_step):
                tile_step(2 * t)
                tile_step(2 * t + 1)
                return 0

            lax.fori_loop(0, tiles // 2, two_tiles, 0)
            at = pl.ds(group.start, SUBLANES), slice(None), pl.ds(row0, SUBLANES)
            for stage, hbm in ((fwd_stage, fwd_hbm), (adj_stage, adj_hbm)):
                copies.append(pltpu.make_async_copy(stage.at[at], hbm.at[at], sems.at[len(copies)]))
                copies[-1].start()
    for copy in copies:
        copy.wait()


def finish(scalars, sums, forward_parts, adjoint_parts, line, total_rows):
    x, z, u = forward_parts
    rows, parts, waves, width = x.shape[0] - 2 * HALO, *x.shape[1:]
    field = array(waves, parts, rows, width)
    stage = pltpu.VMEM((waves, parts, rows, width), jnp.float32)
    return pl.pallas_call(
        functools.partial(finish_kernel, total_rows=total_rows),
        in_specs=[SMEM] * 2 + [VMEM] * 8,
        out_specs=[HBM, HBM, VMEM, VMEM, VMEM],
        out_shape=[field, field, array(rows, width), array(*z.shape), array(*u.shape)],
        scratch_shapes=[
            pltpu.VMEM((11, waves, LANES), jnp.float32),
            stage,
            stage,
            pltpu.SemaphoreType.DMA((8,)),
        ],
        input_output_aliases={7: 3, 8: 4},
        compiler_params=pltpu.CompilerParams(vmem_limit_bytes=FINISH_LIMIT),
        name="finish",
    )(*scalars, sums, *forward_parts, *adjoint_parts, line)[:3]


def step_lengths(rr, rv_re, rv_im, vv, wr_re, wr_im, wv_re, wv_im, ww):
    half = floor_share * rr
    bounded = jnp.maximum(rv_re * rv_re + rv_im * rv_im, half * half)
    a_re = rr * rv_re / bounded
    a_im = -rr * rv_im / bounded
    a_sq = a_re * a_re + a_im * a_im
    ts_re = rv_re - a_re * vv - (a_re * wr_re + a_im * wr_im) + a_sq * wv_re
    ts_im = -rv_im - a_im * vv - (a_re * wr_im - a_im * wr_re) + a_sq * wv_im
    tt = vv - 2.0 * (a_re * wv_re + a_im * wv_im) + a_sq * ww
    o_re = ts_re / tt
    o_im = ts_im / tt
    return (a_re + o_re, a_im + o_im, a_im * o_im - a_re * o_re, -(a_re * o_im + a_im * o_re))


def with_line(base, line, b_re, b_im):
    rr, rv_re, rv_im, vv, wr_re, wr_im, wv_re, wv_im, ww = base
    b_sq = b_re * b_re + b_im * b_im

    def pair(at):
        return line[at], line[at + 1]

    def times(p):
        return b_re * p[0] - b_im * p[1], b_re * p[1] + b_im * p[0]

    def times_conj(p):
        return b_re * p[0] + b_im * p[1], b_re * p[1] - b_im * p[0]

    def mixed(re, im, forth, back, both):
        f, h = times(forth), times_conj(back)
        return re + f[0] + h[0] + b_sq * both[0], im + f[1] + h[1] + b_sq * both[1]

    def square(value, cross, both):
        return value + 2.0 * times(cross)[0] + b_sq * both

    rv_re, rv_im = mixed(rv_re, rv_im, pair(7), pair(18), pair(20))
    wr_re, wr_im = mixed(wr_re, wr_im, pair(22), pair(0), pair(24))
    wv_re, wv_im = mixed(wv_re, wv_im, pair(11), pair(2), pair(13))
    rr = square(rr, pair(16), line[26])
    vv = square(vv, pair(9), line[15])
    ww = square(ww, pair(4), line[6])
    return rr, rv_re, rv_im, vv, wr_re, wr_im, wv_re, wv_im, ww


def local(
    warm_field,
    warm_adjoint,
    permittivity,
    design_mask,
    source_row,
    monitor_row,
    wavenumber,
    bloch_phase,
    source_profile,
    monitor_profile,
):
    rows = permittivity.shape[0]
    count = lax.axis_size("gx")
    index = lax.axis_index("gx")
    total_rows = rows * count
    first_row = (index * rows).astype(jnp.int32).reshape(1)
    pairing_one = [(i, i ^ 1) for i in range(count)]
    pairing_two = [(i, (i + 1 if i % 2 else i - 1) % count) for i in range(count)]
    fwd_first, fwd_second = outer_rows(first_row, warm_field, permittivity)
    fwd_got = (
        lax.ppermute(fwd_first, "gx", pairing_one),
        lax.ppermute(fwd_second, "gx", pairing_two),
    )
    adj_first, adj_second = outer_rows(first_row, warm_adjoint)
    adj_got = (
        lax.ppermute(adj_first, "gx", pairing_one),
        lax.ppermute(adj_second, "gx", pairing_two),
    )
    scalars = (
        jnp.concatenate([first_row, source_row, monitor_row]),
        jnp.concatenate([wavenumber, jnp.cos(bloch_phase), jnp.sin(bloch_phase)]),
    )
    fx, fz, fu, f_sums, diag, inv = inner_rows(
        True, warm_field, scalars, (permittivity, source_profile), total_rows
    )
    ax, az, au, a_sums = inner_rows(False, warm_adjoint, scalars, (diag, inv), total_rows)
    fx, fz, fu, diag, inv, f_sums = outer_rows_solve(
        True,
        scalars,
        fwd_got,
        (fx, fz, fu, f_sums, diag, inv),
        (source_profile, monitor_profile),
        count,
        total_rows,
    )
    ax, az, au, sums, line = outer_rows_solve(
        False,
        scalars,
        adj_got,
        (ax, az, au, a_sums, diag, inv),
        (monitor_profile, f_sums),
        count,
        total_rows,
    )
    forward, adjoint, partial = finish(
        scalars,
        lax.all_to_all(sums, "gx", 0, 0, tiled=True),
        (fx, fz, fu),
        (ax, az, au),
        line,
        total_rows,
    )
    summed_terms = lax.all_gather(partial, "wa").sum(axis=0)
    gradient = design_mask.astype(jnp.float32) * summed_terms
    return (forward, adjoint, gradient)


def solution(mesh):
    placed = (
        P("wa", None, "gx", None),
        P("wa", None, "gx", None),
        P("gx", None),
        P("gx", None),
        P("wa"),
        P("wa"),
        P("wa"),
        P("wa"),
        P("wa", None, None),
        P("wa", None, None),
    )
    return jax.shard_map(
        local,
        mesh=mesh,
        in_specs=placed,
        out_specs=(P("wa", None, "gx", None), P("wa", None, "gx", None), P("gx", None)),
        check_vma=False,
    )
```

```python
import functools

import jax
import jax.numpy as jnp
from jax import lax
from jax.experimental import pallas as pl
from jax.experimental.pallas import tpu as pltpu
from jax.sharding import PartitionSpec as P

floor_share = 0.5
LANES = 128
SUBLANES = 8
HALO = 3
EPS_ROWS = 2
BASE_SUMS = 9
MARK_SUMS = 6
LINE_SUMS = 27
FWD_SUMS = BASE_SUMS + MARK_SUMS
GROUP_LANES = 64
TABLE_COLUMNS = 7
INNER_LIMIT = 2 * 2**20
OUTER_LIMIT = 4 * 2**20
FINISH_LIMIT = 10 * 2**20
VMEM = pl.BlockSpec(memory_space=pltpu.VMEM)
SMEM = pl.BlockSpec(memory_space=pltpu.SMEM)
HBM = pl.BlockSpec(memory_space=pltpu.HBM)


def lane_slice(j):
    return slice(j * LANES, (j + 1) * LANES)


def is_odd(first_row_ref, rows):
    return lax.rem(first_row_ref[0], 2 * rows) != 0


def pack_kernel(first_row_ref, field_ref, *refs, with_eps):
    if with_eps:
        eps_ref, first_ref, second_ref = refs
    else:
        first_ref, second_ref = refs
    waves, parts, rows, width = field_ref.shape
    odd = is_odd(first_row_ref, rows)
    pieces = [
        (slice(wave0, wave0 + SUBLANES), part)
        for wave0 in range(0, waves, SUBLANES)
        for part in range(parts)
    ]
    if with_eps:
        at = HALO * parts * waves
        low = jnp.tile(eps_ref[:EPS_ROWS, :], (SUBLANES // EPS_ROWS, 1))
        high = jnp.tile(eps_ref[rows - EPS_ROWS :, :], (SUBLANES // EPS_ROWS, 1))
        first_ref[at : at + SUBLANES, :] = jnp.where(odd, low, high)
        second_ref[at : at + SUBLANES, :] = jnp.where(odd, high, low)
    for group, part in pieces:
        for lane0 in range(0, width, LANES):
            lanes = slice(lane0, lane0 + LANES)
            head = jnp.swapaxes(field_ref[group, part, :SUBLANES, lanes], 0, 1)
            tail = jnp.swapaxes(field_ref[group, part, rows - SUBLANES :, lanes], 0, 1)
            for k in range(HALO):
                at = (k * parts + part) * waves + group.start
                low = head[k]
                high = tail[SUBLANES - HALO + k]
                first_ref[at : at + SUBLANES, lanes] = jnp.where(odd, low, high)
                second_ref[at : at + SUBLANES, lanes] = jnp.where(odd, high, low)


def outer_rows(first_row, field, eps=None):
    waves, parts, rows, width = field.shape
    height = HALO * parts * waves + (0 if eps is None else SUBLANES)
    shape = jax.ShapeDtypeStruct((height, width), jnp.float32)
    return pl.pallas_call(
        functools.partial(pack_kernel, with_eps=eps is not None),
        in_specs=[SMEM, VMEM] + ([] if eps is None else [VMEM]),
        out_specs=[VMEM, VMEM],
        out_shape=[shape, shape],
        compiler_params=pltpu.CompilerParams(
            vmem_limit_bytes=INNER_LIMIT
        ),
        name="outer_rows",
    )(first_row, field, *(() if eps is None else (eps,)))


def lane_neighbours(load, count):
    lane = lax.broadcasted_iota(jnp.int32, (SUBLANES, LANES), 1)
    at_low = lane == 0
    at_high = lane == LANES - 1
    zero = jnp.zeros((SUBLANES, LANES), jnp.float32)
    tile = load(0)
    up_before = zero
    down_here = pltpu.roll(tile, LANES - 1, 1)
    for j in range(count):
        up_here = pltpu.roll(tile, 1, 1)
        if j + 1 < count:
            following = load(j + 1)
            down_after = pltpu.roll(following, LANES - 1, 1)
        else:
            following, down_after = None, zero
        yield (
            j,
            tile,
            jnp.where(at_low, up_before, up_here) + jnp.where(at_high, down_after, down_here),
        )
        tile, up_before, down_here = following, up_here, down_after


class Scalars:
    def __init__(self, whole_ref, real_ref):
        self.whole, self.real = whole_ref, real_ref
        self.waves = real_ref.shape[0] // 3
        self.first_row = whole_ref[0]

    def source(self, w):
        return self.whole[1 + w]

    def monitor(self, w):
        return self.whole[1 + self.waves + w]

    def squared_k(self, w):
        return self.real[w]

    def cosine(self, w):
        return self.real[self.waves + w]

    def sine(self, w):
        return self.real[2 * self.waves + w]


class Rows:
    def __init__(self, x_ref, z_ref, u_ref, diag_ref, inv_ref, wave_ref):
        self.x, self.z, self.u = x_ref, z_ref, u_ref
        self.diag, self.inv, self.wave = diag_ref, inv_ref, wave_ref
        _, self.parts, self.waves, width = z_ref.shape
        self.rows = z_ref.shape[0] - 4
        self.tiles = width // LANES

    def groups(self):
        return [slice(w, w + SUBLANES) for w in range(0, self.waves, SUBLANES)]

    def column(self, index, group):
        return self.wave[index, group, :]

    def set_diagonal(self, i, eps_row):
        for group in self.groups():
            squared_k = self.column(0, group)
            for j in range(self.tiles):
                lanes = lane_slice(j)
                diagonal = 4.0 - squared_k * jnp.broadcast_to(eps_row(lanes), (SUBLANES, LANES))
                self.diag[i, group, lanes] = diagonal
                self.inv[i, group, lanes] = 1.0 / diagonal

    def tiles_of(self, ref, i, count, group):
        chains = [
            [
                lane_neighbours(
                    lambda j, at=i + k, part=part: ref[at, part, group, lane_slice(j)], self.tiles
                )
                for part in range(self.parts)
            ]
            for k in range(count)
        ]
        for j in range(self.tiles):
            lanes = lane_slice(j)
            now = [[next(chain)[1:] for chain in row] for row in chains]
            out = []
            for k in range(count):
                row = []
                for part in range(self.parts):
                    low = now[k - 1][part][0] if k else ref[i - 1, part, group, lanes]
                    high = now[k + 1][part][0] if k + 1 < count else ref[i + count, part, group, lanes]
                    centre, sides = now[k][part]
                    row.append((centre, low + high, sides))
                out.append(row)
            yield j, out

    def residual(self, i, count):
        for group in self.groups():
            for j, block in self.tiles_of(self.x, i + 1, count, group):
                lanes = lane_slice(j)
                for k in range(count):
                    diagonal = self.diag[i + k, group, lanes]
                    inverse = self.inv[i + k, group, lanes]
                    for part, (centre, around, sides) in enumerate(block[k]):
                        self.z[i + k, part, group, lanes] = (
                            around + sides - diagonal * centre
                        ) * inverse

    def image(self, i, count):
        for group in self.groups():
            for j, block in self.tiles_of(self.z, i + 1, count, group):
                lanes = lane_slice(j)
                for k in range(count):
                    inverse = self.inv[i + 1 + k, group, lanes]
                    for part, (centre, around, sides) in enumerate(block[k]):
                        self.u[i + k, part, group, lanes] = centre - (around + sides) * inverse

    def vectors(self, i, group, count=1):
        for j, block in self.tiles_of(self.u, i + 1, count, group):
            lanes = lane_slice(j)
            for k in range(count):
                diagonal = self.diag[i + 2 + k, group, lanes]
                r, v, w = [], [], []
                for part, (centre, around, sides) in enumerate(block[k]):
                    r.append(diagonal * self.z[i + 2 + k, part, group, lanes])
                    v.append(diagonal * centre)
                    w.append(v[-1] - (around + sides))
                yield j, r, v, w

    def twice(self, i, group, sums, count):
        rr, rv_re, rv_im, vv, wr_re, wr_im, wv_re, wv_im, ww = sums
        for _, r, v, w in self.vectors(i, group, count):
            rr += r[0] * r[0] + r[1] * r[1]
            rv_re += r[0] * v[0] + r[1] * v[1]
            rv_im += r[0] * v[1] - r[1] * v[0]
            vv += v[0] * v[0] + v[1] * v[1]
            wr_re += w[0] * r[0] + w[1] * r[1]
            wr_im += w[0] * r[1] - w[1] * r[0]
            wv_re += w[0] * v[0] + w[1] * v[1]
            wv_im += w[0] * v[1] - w[1] * v[0]
            ww += w[0] * w[0] + w[1] * w[1]
        return rr, rv_re, rv_im, vv, wr_re, wr_im, wv_re, wv_im, ww

    def any_at(self, row_of, row):
        hit = row_of(0) == row
        for w in range(1, self.waves):
            hit = jnp.logical_or(hit, row_of(w) == row)
        return hit

    def source(self, i, scalars, total_rows, side_ref):
        row = scalars.first_row + i - 2
        row = jnp.where(row < 0, row + total_rows, row)
        row = jnp.where(row >= total_rows, row - total_rows, row)

        @pl.when(self.any_at(scalars.source, row))
        def _():
            for group in self.groups():
                cosine, sine = self.frame(i - 2, group)
                chosen = self.column(5, group) == row.astype(jnp.float32)
                for j in range(self.tiles):
                    lanes = lane_slice(j)
                    re = side_ref[group, 0, lanes]
                    im = side_ref[group, 1, lanes]
                    inverse = self.inv[i, group, lanes]
                    self.z[i, 0, group, lanes] += jnp.where(
                        chosen, (cosine * re - sine * im) * inverse, 0.0
                    )
                    self.z[i, 1, group, lanes] += jnp.where(
                        chosen, (sine * re + cosine * im) * inverse, 0.0
                    )

    def frame(self, row, group):
        below = row < 0
        above = row >= self.rows
        return (
            jnp.where(below, self.column(1, group), jnp.where(above, self.column(3, group), 1.0)),
            jnp.where(below, self.column(2, group), jnp.where(above, self.column(4, group), 0.0)),
        )


def wave_column(value_of, wave0):
    sublane = lax.broadcasted_iota(jnp.int32, (SUBLANES, LANES), 0)
    out = jnp.zeros((SUBLANES, LANES), jnp.float32)
    for k in range(SUBLANES):
        out = jnp.where(sublane == k, value_of(wave0 + k).astype(jnp.float32), out)
    return out


def fill_table(table_ref, scalars, rows, total_rows, sign):
    at_first = scalars.first_row == 0
    at_last = scalars.first_row == total_rows - rows
    for wave0 in range(0, table_ref.shape[1], SUBLANES):
        group = slice(wave0, wave0 + SUBLANES)
        cosine = wave_column(scalars.cosine, wave0)
        sine = sign * wave_column(scalars.sine, wave0)
        table_ref[0, group, :] = wave_column(scalars.squared_k, wave0)
        table_ref[1, group, :] = jnp.where(at_first, cosine, 1.0)
        table_ref[2, group, :] = jnp.where(at_first, -sine, 0.0)
        table_ref[3, group, :] = jnp.where(at_last, cosine, 1.0)
        table_ref[4, group, :] = jnp.where(at_last, sine, 0.0)
        table_ref[5, group, :] = wave_column(scalars.source, wave0)
        table_ref[6, group, :] = wave_column(scalars.monitor, wave0)


def lanes_of(out, totals, wave0, offset):
    lane = lax.broadcasted_iota(jnp.int32, (SUBLANES, LANES), 1)
    base = wave0 // SUBLANES * GROUP_LANES + offset
    for n, total in enumerate(totals):
        out = jnp.where(lane == base + n, jnp.sum(total, axis=1, keepdims=True), out)
    return out


def inner_kernel(*refs, forward, total_rows):
    scalars = Scalars(*refs[:2])
    field_ref, refs = refs[2], refs[3:]
    if forward:
        (eps_ref, side_ref) = refs[:2]
        (x_ref, z_ref, u_ref, sums_ref, diag_ref, inv_ref, table_ref) = refs[2:]
    else:
        (diag_ref, inv_ref) = refs[:2]
        (x_ref, z_ref, u_ref, sums_ref, table_ref) = refs[2:]
    step = Rows(x_ref, z_ref, u_ref, diag_ref, inv_ref, table_ref)
    rows, waves = step.rows, step.waves
    fill_table(table_ref, scalars, rows, total_rows, 1.0 if forward else -1.0)
    if forward:
        for row in range(rows):
            step.set_diagonal(row + 2, lambda lanes, row=row: eps_ref[row : row + 1, lanes])
    def turn(j, _):
        lanes = pl.ds(pl.multiple_of(j * LANES, LANES), LANES)
        for part in range(step.parts):
            for group in step.groups():
                for row0 in range(0, rows, SUBLANES):
                    x_ref[HALO + row0 : HALO + row0 + SUBLANES, part, group, lanes] = (
                        jnp.swapaxes(
                            field_ref[group, part, row0 : row0 + SUBLANES, lanes], 0, 1
                        )
                    )
        return 0

    lax.fori_loop(0, step.tiles, turn, 0)

    def residual(t, _):
        i = 3 + 2 * t
        step.residual(i, 2)
        if forward:
            step.source(i, scalars, total_rows, side_ref)
            step.source(i + 1, scalars, total_rows, side_ref)
        return 0

    def image(t, _):
        step.image(3 + 3 * t, 3)
        return 0

    lax.fori_loop(0, (rows - 2) // 2, residual, 0)
    lax.fori_loop(0, (rows - 4) // 3, image, 0)
    zero = jnp.zeros((SUBLANES, LANES), jnp.float32)
    out = zero
    for group in step.groups():
        sums = lax.fori_loop(
            0,
            (rows - 6) // 2,
            lambda t, sums, group=group: step.twice(3 + 2 * t, group, sums, 2),
            (zero,) * BASE_SUMS,
        )
        out = lanes_of(out, sums, group.start, 0 if forward else FWD_SUMS)
    sums_ref[...] = out


def outer_kernel(*refs, forward, total_rows):
    scalars = Scalars(*refs[:2])
    first_ref, second_ref, refs = refs[2], refs[3], refs[4:]
    if forward:
        (part_ref, _, _, _, _, _, side_ref, mark_ref) = refs[:8]
        (x_ref, z_ref, u_ref, diag_ref, inv_ref, sums_ref, table_ref, mark_sums) = refs[8:]
    else:
        (part_ref, _, _, _, diag_ref, inv_ref, line_ref, inner_line_sums, fwd_sums_ref) = refs[:9]
        (x_ref, z_ref, u_ref, sums_ref, table_ref, line_sums) = refs[9:]
    step = Rows(x_ref, z_ref, u_ref, diag_ref, inv_ref, table_ref)
    rows, parts, waves, tiles = step.rows, step.parts, step.waves, step.tiles
    first_row = scalars.first_row
    odd = lax.rem(first_row, 2 * rows) != 0
    fill_table(table_ref, scalars, rows, total_rows, 1.0 if forward else -1.0)
    for group in step.groups():
        for base, offset, swap in ((0, 1, False), (HALO + rows, 3, True)):
            cosine = step.column(offset, group)
            sine = step.column(offset + 1, group)
            for k in range(HALO):
                for j in range(tiles):
                    lanes = lane_slice(j)
                    values = []
                    for part in range(parts):
                        at = (k * parts + part) * waves + group.start
                        one = first_ref[at : at + SUBLANES, lanes]
                        two = second_ref[at : at + SUBLANES, lanes]
                        values.append(jnp.where(odd, two, one) if swap else jnp.where(odd, one, two))
                    re, im = values
                    x_ref[base + k, 0, group, lanes] = cosine * re - sine * im
                    x_ref[base + k, 1, group, lanes] = sine * re + cosine * im
    if forward:
        at = HALO * parts * waves
        for k in range(EPS_ROWS):

            def above_eps(lanes, k=k):
                row = slice(at + k, at + k + 1)
                return jnp.where(odd, first_ref[row, lanes], second_ref[row, lanes])

            def below_eps(lanes, k=k):
                row = slice(at + k, at + k + 1)
                return jnp.where(odd, second_ref[row, lanes], first_ref[row, lanes])

            step.set_diagonal(k, above_eps)
            step.set_diagonal(rows + 2 + k, below_eps)

    def residual(t, _):
        i = t * (rows + 1)
        step.residual(i, 3)
        if forward:
            for k in range(3):
                step.source(i + k, scalars, total_rows, side_ref)
        return 0

    def image(t, _):
        step.image(t * (rows - 1), 3)
        return 0

    lax.fori_loop(0, 2, residual, 0)
    lax.fori_loop(0, 2, image, 0)
    zero = jnp.zeros((SUBLANES, LANES), jnp.float32)
    base_sums = []
    for group in step.groups():
        base_sums.append(
            lax.fori_loop(
                0,
                2,
                lambda t, sums, group=group: step.twice(t * (rows - 3), group, sums, 3),
                (zero,) * BASE_SUMS,
            )
        )
    if forward:
        mark_sums[...] = jnp.zeros_like(mark_sums)

        def mark_at(i, _):
            row = first_row + i

            @pl.when(step.any_at(scalars.monitor, row))
            def _():
                for group in step.groups():
                    chosen = step.column(6, group) == row.astype(jnp.float32)
                    for j in range(tiles):
                        lanes = lane_slice(j)
                        m_re = jnp.where(chosen, mark_ref[group, 0, lanes], 0.0)
                        m_im = jnp.where(chosen, mark_ref[group, 1, lanes], 0.0)
                        for n, (ref, shift) in enumerate(((x_ref, 3), (z_ref, 2), (u_ref, 1))):
                            f_re = ref[i + shift, 0, group, lanes]
                            f_im = ref[i + shift, 1, group, lanes]
                            mark_sums[2 * n, group] += m_re * f_re + m_im * f_im
                            mark_sums[2 * n + 1, group] += m_re * f_im - m_im * f_re

            return 0

        lax.fori_loop(0, rows, mark_at, 0)
        extra, count = mark_sums, MARK_SUMS
    else:
        line_products(
            step,
            scalars,
            total_rows,
            line_ref,
            line_sums,
            lambda row: jnp.logical_and(
                jnp.logical_and(row >= 0, row < rows),
                jnp.logical_or(row < 3, row >= rows - 3),
            ),
        )
        line_sums[...] += inner_line_sums[...]
        extra, count = line_sums, LINE_SUMS
    out = part_ref[...]
    new = jnp.zeros((SUBLANES, LANES), jnp.float32)
    for n, group in enumerate(step.groups()):
        more = list(base_sums[n]) + [extra[k, group] for k in range(count)]
        new = lanes_of(new, more, group.start, 0 if forward else FWD_SUMS)
    out = out + new
    if forward:
        sums_ref[...] = out
    else:
        out = out + fwd_sums_ref[...]
        for n in range(sums_ref.shape[0]):
            sums_ref[n] = out


def distance_to(row, first_row, total_rows):
    away = row - first_row
    away = jnp.where(away >= total_rows - 2, away - total_rows, away)
    return jnp.where(away < -2, away + total_rows, away)


def dot(a, b):
    return a[0] * b[0] + a[1] * b[1], a[0] * b[1] - a[1] * b[0]


def line_waves(step, scalars, total_rows, body):
    def one_wave(w, _):
        away = distance_to(scalars.monitor(w), scalars.first_row, total_rows)

        @pl.when(away <= step.rows + 1)
        def _():
            group = pl.ds(pl.multiple_of((w // SUBLANES) * SUBLANES, SUBLANES), SUBLANES)
            sublane = lax.broadcasted_iota(jnp.int32, (SUBLANES, LANES), 0)
            body(away, group, sublane == w % SUBLANES)

        return 0

    lax.fori_loop(0, step.waves, one_wave, 0)


def line_plane(line_ref, n, part, group, mine):
    return lambda j: jnp.where(mine, line_ref[n, part, group, lane_slice(j)], 0.0)


def line_fields(step, scalars, total_rows, mark_ref, line_ref):
    rows, tiles = step.rows, step.tiles
    line_ref[...] = jnp.zeros_like(line_ref)

    def body(away, group, mine):
        cosine, sine = step.frame(away, group)
        before = jnp.maximum(away + 1, 0)
        after = jnp.minimum(away + 3, rows + 3)
        for j in range(tiles):
            lanes = lane_slice(j)
            m_re = jnp.where(mine, mark_ref[group, 0, lanes], 0.0)
            m_im = jnp.where(mine, mark_ref[group, 1, lanes], 0.0)
            g = (cosine * m_re + sine * m_im, sine * m_re - cosine * m_im)
            for part in range(2):
                z = g[part] * step.inv[away + 2, group, lanes]
                line_ref[0, part, group, lanes] += z
                line_ref[1, part, group, lanes] -= z * step.inv[before, group, lanes]
                line_ref[3, part, group, lanes] -= z * step.inv[after, group, lanes]
                line_ref[4, part, group, lanes] += g[part]
        for part in range(2):
            for j, _, sides in lane_neighbours(line_plane(line_ref, 0, part, group, mine), tiles):
                lanes = lane_slice(j)
                image = line_plane(line_ref, 4, part, group, mine)(j) - sides
                line_ref[5, part, group, lanes] += image
                line_ref[2, part, group, lanes] += image * step.inv[away + 2, group, lanes]

    line_waves(step, scalars, total_rows, body)


def line_products(step, scalars, total_rows, line_ref, line_sums, counts):
    line_sums[...] = jnp.zeros_like(line_sums)

    def body(away, group, mine):
        for k in range(-2, 3):

            @pl.when(counts(away + k))
            def _(k=k):
                zero = jnp.zeros((SUBLANES, LANES), jnp.float32)
                totals = [zero] * LINE_SUMS

                def add(at, pair):
                    totals[at] = totals[at] + pair[0]
                    totals[at + 1] = totals[at + 1] + pair[1]

                if abs(k) < 2:
                    sides_of = [
                        [
                            sides
                            for _, _, sides in lane_neighbours(
                                line_plane(line_ref, 2 + k, part, group, mine), step.tiles
                            )
                        ]
                        for part in range(2)
                    ]
                for j, r, v, w_vec in step.vectors(away + k, group):
                    get = lambda n: [
                        line_plane(line_ref, n, part, group, mine)(j) for part in range(2)
                    ]
                    if abs(k) == 2:
                        wg = [-t for t in get(1 if k < 0 else 3)]
                    elif abs(k) == 1:
                        vg = [-t for t in get(0)]
                        mid = get(2)
                        wg = [vg[p] - mid[p] - sides_of[p][j] for p in range(2)]
                    else:
                        g, vg, low, high = get(4), get(5), get(1), get(3)
                        wg = [vg[p] - (low[p] + high[p]) - sides_of[p][j] for p in range(2)]
                    add(0, dot(wg, r))
                    add(2, dot(wg, v))
                    add(4, dot(w_vec, wg))
                    totals[6] = totals[6] + dot(wg, wg)[0]
                    if abs(k) < 2:
                        add(7, dot(r, vg))
                        add(9, dot(v, vg))
                        add(11, dot(w_vec, vg))
                        add(13, dot(wg, vg))
                        totals[15] = totals[15] + dot(vg, vg)[0]
                    if k == 0:
                        add(16, dot(r, g))
                        add(18, dot(g, v))
                        add(20, dot(g, vg))
                        add(22, dot(w_vec, g))
                        add(24, dot(wg, g))
                        totals[26] = totals[26] + dot(g, g)[0]
                used = 7 if abs(k) == 2 else 16 if abs(k) == 1 else LINE_SUMS
                for n in range(used):
                    line_sums[n, group] += totals[n]

    line_waves(step, scalars, total_rows, body)


def line_kernel(
    whole_ref,
    real_ref,
    z_ref,
    u_ref,
    diag_ref,
    inv_ref,
    mark_ref,
    line_ref,
    line_sums,
    table_ref,
    *,
    total_rows,
):
    scalars = Scalars(whole_ref, real_ref)
    step = Rows(None, z_ref, u_ref, diag_ref, inv_ref, table_ref)
    fill_table(table_ref, scalars, step.rows, total_rows, -1.0)
    line_fields(step, scalars, total_rows, mark_ref, line_ref)
    line_products(
        step,
        scalars,
        total_rows,
        line_ref,
        line_sums,
        lambda row: jnp.logical_and(row >= 3, row < step.rows - 3),
    )


def inner_lines(scalars, z, u, diag, inv, profile, total_rows):
    _, parts, waves, width = z.shape
    return pl.pallas_call(
        functools.partial(line_kernel, total_rows=total_rows),
        in_specs=[SMEM] * 2 + [VMEM] * 5,
        out_specs=[VMEM, VMEM],
        out_shape=[array(6, parts, waves, width), array(LINE_SUMS, waves, LANES)],
        scratch_shapes=[pltpu.VMEM((TABLE_COLUMNS, waves, LANES), jnp.float32)],
        compiler_params=pltpu.CompilerParams(vmem_limit_bytes=INNER_LIMIT),
        name="adjoint_line",
    )(*scalars, z, u, diag, inv, profile)


def array(*shape):
    return jax.ShapeDtypeStruct(shape, jnp.float32)


def inner_rows(forward, field, scalars, extra, total_rows):
    waves, parts, rows, width = field.shape
    args = (*scalars, field, *extra)
    out_shape = [
        array(rows + 6, parts, waves, width),
        array(rows + 4, parts, waves, width),
        array(rows + 2, parts, waves, width),
        array(SUBLANES, LANES),
    ]
    if forward:
        out_shape += [array(rows + 4, waves, width)] * 2
    return pl.pallas_call(
        functools.partial(inner_kernel, forward=forward, total_rows=total_rows),
        in_specs=[SMEM] * 2 + [VMEM, VMEM, VMEM],
        out_specs=[VMEM] * len(out_shape),
        out_shape=out_shape,
        scratch_shapes=[
            pltpu.VMEM((TABLE_COLUMNS, waves, LANES), jnp.float32),
        ],
        compiler_params=pltpu.CompilerParams(
            vmem_limit_bytes=INNER_LIMIT
        ),
        name="forward_inner" if forward else "adjoint_inner",
    )(*args)


def outer_rows_solve(forward, scalars, received, inner, more, copies, total_rows):
    x, z, u, sums, diag, inv = inner
    waves = x.shape[2]
    args = (*scalars, *received, sums, x, z, u, diag, inv, *more)
    scratch = [pltpu.VMEM((TABLE_COLUMNS, waves, LANES), jnp.float32)]
    if forward:
        out_shape = [array(*a.shape) for a in (x, z, u, diag, inv, sums)]
        aliases = {5: 0, 6: 1, 7: 2, 8: 3, 9: 4}
        scratch += [pltpu.VMEM((MARK_SUMS, waves, LANES), jnp.float32)]
    else:
        out_shape = [array(*a.shape) for a in (x, z, u)] + [array(copies, SUBLANES, LANES)]
        aliases = {5: 0, 6: 1, 7: 2}
        scratch += [pltpu.VMEM((LINE_SUMS, waves, LANES), jnp.float32)]
    return pl.pallas_call(
        functools.partial(outer_kernel, forward=forward, total_rows=total_rows),
        in_specs=[SMEM] * 2 + [VMEM] * (len(args) - 2),
        out_specs=[VMEM] * len(out_shape),
        out_shape=out_shape,
        scratch_shapes=scratch,
        input_output_aliases=aliases,
        compiler_params=pltpu.CompilerParams(vmem_limit_bytes=OUTER_LIMIT),
        name="forward_outer" if forward else "adjoint_outer",
    )(*args)


def finish_kernel(
    whole_ref,
    real_ref,
    sums_ref,
    xf_ref,
    zf_ref,
    uf_ref,
    xa_ref,
    _z_in,
    _u_in,
    line_ref,
    fwd_hbm,
    adj_hbm,
    grad_ref,
    za_ref,
    ua_ref,
    coef_ref,
    fwd_stage,
    adj_stage,
    sems,
    *,
    total_rows,
):
    waves, parts, rows, width = fwd_hbm.shape
    tiles = width // LANES
    groups = [slice(w, w + SUBLANES) for w in range(0, waves, SUBLANES)]
    scalars = Scalars(whole_ref, real_ref)

    def column(index, group):
        return coef_ref[index, group, :]

    sums = jnp.sum(sums_ref[...], axis=0)
    for group in groups:
        base = group.start // SUBLANES * GROUP_LANES
        cols = [
            jnp.broadcast_to(sums[:, base + n : base + n + 1], (SUBLANES, LANES))
            for n in range(FWD_SUMS + BASE_SUMS + LINE_SUMS)
        ]
        fwd_coefs = step_lengths(*cols[:BASE_SUMS])
        a_re, a_im, b_re, b_im = fwd_coefs
        s0_re, s0_im, s1_re, s1_im, s2_re, s2_im = cols[BASE_SUMS:FWD_SUMS]
        over_re = s0_re + (a_re * s1_re - a_im * s1_im) + (b_re * s2_re - b_im * s2_im)
        over_im = s0_im + (a_re * s1_im + a_im * s1_re) + (b_re * s2_im + b_im * s2_re)
        adj_cols = cols[FWD_SUMS:]
        adj_coefs = step_lengths(
            *with_line(adj_cols[:BASE_SUMS], adj_cols[BASE_SUMS:], over_re, -over_im)
        )
        twice_k = 2.0 * wave_column(scalars.squared_k, group.start)
        for n, value in enumerate((*fwd_coefs, *adj_coefs, twice_k, over_re, -over_im)):
            coef_ref[n, group, :] = value

    def one_wave(w, _):
        away = distance_to(scalars.monitor(w), scalars.first_row, total_rows)

        @pl.when(away <= rows)
        def _():
            group = pl.ds(pl.multiple_of((w // SUBLANES) * SUBLANES, SUBLANES), SUBLANES)
            mine = lax.broadcasted_iota(jnp.int32, (SUBLANES, LANES), 0) == w % SUBLANES
            b_re = jnp.where(mine, column(9, group), 0.0)
            b_im = jnp.where(mine, column(10, group), 0.0)
            for n, (ref, shift, k) in enumerate(
                ((za_ref, 2, 0), (ua_ref, 1, -1), (ua_ref, 1, 0), (ua_ref, 1, 1))
            ):

                @pl.when(jnp.logical_and(away + k >= 0, away + k < rows))
                def _(n=n, ref=ref, at=away + k + shift):
                    for j in range(tiles):
                        lanes = lane_slice(j)
                        re = line_ref[n, 0, group, lanes]
                        im = line_ref[n, 1, group, lanes]
                        ref[at, 0, group, lanes] += b_re * re - b_im * im
                        ref[at, 1, group, lanes] += b_re * im + b_im * re

        return 0

    lax.fori_loop(0, waves, one_wave, 0)
    sublane = lax.broadcasted_iota(jnp.int32, (SUBLANES, LANES), 0)

    copies = []
    for row0 in range(0, rows, SUBLANES):
        for group in groups:

            def tile_step(j, row0=row0, group=group):
                lanes = pl.ds(pl.multiple_of(j * LANES, LANES), LANES)
                coefs = [column(n, group) for n in range(9)]
                results = [[], [], [], []]
                out = jnp.zeros((SUBLANES, LANES), jnp.float32)
                for k in range(SUBLANES):
                    row = row0 + k
                    values = []
                    for base, x_ref, z_ref, u_ref in (
                        (0, xf_ref, zf_ref, uf_ref),
                        (4, xa_ref, za_ref, ua_ref),
                    ):
                        a_re, a_im, b_re, b_im = coefs[base : base + 4]
                        z_re = z_ref[row + 2, 0, group, lanes]
                        z_im = z_ref[row + 2, 1, group, lanes]
                        u_re = u_ref[row + 1, 0, group, lanes]
                        u_im = u_ref[row + 1, 1, group, lanes]
                        values.append(
                            x_ref[row + HALO, 0, group, lanes]
                            + (a_re * z_re - a_im * z_im)
                            + (b_re * u_re - b_im * u_im)
                        )
                        values.append(
                            x_ref[row + HALO, 1, group, lanes]
                            + (a_re * z_im + a_im * z_re)
                            + (b_re * u_im + b_im * u_re)
                        )
                    f_re, f_im, g_re, g_im = values
                    term = coefs[8] * (g_re * f_re - g_im * f_im)
                    out = jnp.where(sublane == k, jnp.sum(term, axis=0, keepdims=True), out)
                    for n in range(4):
                        results[n].append(values[n])
                for n, (ref, part) in enumerate(
                    ((fwd_stage, 0), (fwd_stage, 1), (adj_stage, 0), (adj_stage, 1))
                ):
                    ref[group, part, row0 : row0 + SUBLANES, lanes] = jnp.swapaxes(
                        jnp.stack(results[n]), 0, 1
                    )
                if group.start:
                    out = out + grad_ref[row0 : row0 + SUBLANES, lanes]
                grad_ref[row0 : row0 + SUBLANES, lanes] = out

            def two_tiles(t, _, tile_step=tile_step):
                tile_step(2 * t)
                tile_step(2 * t + 1)
                return 0

            lax.fori_loop(0, tiles // 2, two_tiles, 0)
            at = pl.ds(group.start, SUBLANES), slice(None), pl.ds(row0, SUBLANES)
            for stage, hbm in ((fwd_stage, fwd_hbm), (adj_stage, adj_hbm)):
                copies.append(pltpu.make_async_copy(stage.at[at], hbm.at[at], sems.at[len(copies)]))
                copies[-1].start()
    for copy in copies:
        copy.wait()


def finish(scalars, sums, forward_parts, adjoint_parts, line, total_rows):
    x, z, u = forward_parts
    rows, parts, waves, width = x.shape[0] - 2 * HALO, *x.shape[1:]
    field = array(waves, parts, rows, width)
    stage = pltpu.VMEM((waves, parts, rows, width), jnp.float32)
    return pl.pallas_call(
        functools.partial(finish_kernel, total_rows=total_rows),
        in_specs=[SMEM] * 2 + [VMEM] * 8,
        out_specs=[HBM, HBM, VMEM, VMEM, VMEM],
        out_shape=[field, field, array(rows, width), array(*z.shape), array(*u.shape)],
        scratch_shapes=[
            pltpu.VMEM((11, waves, LANES), jnp.float32),
            stage,
            stage,
            pltpu.SemaphoreType.DMA((8,)),
        ],
        input_output_aliases={7: 3, 8: 4},
        compiler_params=pltpu.CompilerParams(vmem_limit_bytes=FINISH_LIMIT),
        name="finish",
    )(*scalars, sums, *forward_parts, *adjoint_parts, line)[:3]


def step_lengths(rr, rv_re, rv_im, vv, wr_re, wr_im, wv_re, wv_im, ww):
    half = floor_share * rr
    bounded = jnp.maximum(rv_re * rv_re + rv_im * rv_im, half * half)
    a_re = rr * rv_re / bounded
    a_im = -rr * rv_im / bounded
    a_sq = a_re * a_re + a_im * a_im
    ts_re = rv_re - a_re * vv - (a_re * wr_re + a_im * wr_im) + a_sq * wv_re
    ts_im = -rv_im - a_im * vv - (a_re * wr_im - a_im * wr_re) + a_sq * wv_im
    tt = vv - 2.0 * (a_re * wv_re + a_im * wv_im) + a_sq * ww
    o_re = ts_re / tt
    o_im = ts_im / tt
    return (a_re + o_re, a_im + o_im, a_im * o_im - a_re * o_re, -(a_re * o_im + a_im * o_re))


def with_line(base, line, b_re, b_im):
    rr, rv_re, rv_im, vv, wr_re, wr_im, wv_re, wv_im, ww = base
    b_sq = b_re * b_re + b_im * b_im

    def pair(at):
        return line[at], line[at + 1]

    def times(p):
        return b_re * p[0] - b_im * p[1], b_re * p[1] + b_im * p[0]

    def times_conj(p):
        return b_re * p[0] + b_im * p[1], b_re * p[1] - b_im * p[0]

    def mixed(re, im, forth, back, both):
        f, h = times(forth), times_conj(back)
        return re + f[0] + h[0] + b_sq * both[0], im + f[1] + h[1] + b_sq * both[1]

    def square(value, cross, both):
        return value + 2.0 * times(cross)[0] + b_sq * both

    rv_re, rv_im = mixed(rv_re, rv_im, pair(7), pair(18), pair(20))
    wr_re, wr_im = mixed(wr_re, wr_im, pair(22), pair(0), pair(24))
    wv_re, wv_im = mixed(wv_re, wv_im, pair(11), pair(2), pair(13))
    rr = square(rr, pair(16), line[26])
    vv = square(vv, pair(9), line[15])
    ww = square(ww, pair(4), line[6])
    return rr, rv_re, rv_im, vv, wr_re, wr_im, wv_re, wv_im, ww


def local(
    warm_field,
    warm_adjoint,
    permittivity,
    design_mask,
    source_row,
    monitor_row,
    wavenumber,
    bloch_phase,
    source_profile,
    monitor_profile,
):
    rows = permittivity.shape[0]
    count = lax.axis_size("gx")
    index = lax.axis_index("gx")
    total_rows = rows * count
    first_row = (index * rows).astype(jnp.int32).reshape(1)
    pairing_one = [(i, i ^ 1) for i in range(count)]
    pairing_two = [(i, (i + 1 if i % 2 else i - 1) % count) for i in range(count)]
    fwd_first, fwd_second = outer_rows(first_row, warm_field, permittivity)
    fwd_got = (
        lax.ppermute(fwd_first, "gx", pairing_one),
        lax.ppermute(fwd_second, "gx", pairing_two),
    )
    adj_first, adj_second = outer_rows(first_row, warm_adjoint)
    adj_got = (
        lax.ppermute(adj_first, "gx", pairing_one),
        lax.ppermute(adj_second, "gx", pairing_two),
    )
    scalars = (
        jnp.concatenate([first_row, source_row, monitor_row]),
        jnp.concatenate([wavenumber, jnp.cos(bloch_phase), jnp.sin(bloch_phase)]),
    )
    fx, fz, fu, f_sums, diag, inv = inner_rows(
        True, warm_field, scalars, (permittivity, source_profile), total_rows
    )
    ax, az, au, a_sums = inner_rows(False, warm_adjoint, scalars, (diag, inv), total_rows)
    fx, fz, fu, diag, inv, f_sums = outer_rows_solve(
        True,
        scalars,
        fwd_got,
        (fx, fz, fu, f_sums, diag, inv),
        (source_profile, monitor_profile),
        count,
        total_rows,
    )
    line, line_sums = inner_lines(scalars, az, au, diag, inv, monitor_profile, total_rows)
    ax, az, au, sums = outer_rows_solve(
        False,
        scalars,
        adj_got,
        (ax, az, au, a_sums, diag, inv),
        (line, line_sums, f_sums),
        count,
        total_rows,
    )
    forward, adjoint, partial = finish(
        scalars,
        lax.all_to_all(sums, "gx", 0, 0, tiled=True),
        (fx, fz, fu),
        (ax, az, au),
        line,
        total_rows,
    )
    summed_terms = lax.all_gather(partial, "wa").sum(axis=0)
    gradient = design_mask.astype(jnp.float32) * summed_terms
    return (forward, adjoint, gradient)


def solution(mesh):
    placed = (
        P("wa", None, "gx", None),
        P("wa", None, "gx", None),
        P("gx", None),
        P("gx", None),
        P("wa"),
        P("wa"),
        P("wa"),
        P("wa"),
        P("wa", None, None),
        P("wa", None, None),
    )
    return jax.shard_map(
        local,
        mesh=mesh,
        in_specs=placed,
        out_specs=(P("wa", None, "gx", None), P("wa", None, "gx", None), P("gx", None)),
        check_vma=False,
    )
```

```python
import functools

import jax
import jax.numpy as jnp
from jax import lax
from jax.experimental import pallas as pl
from jax.experimental.pallas import tpu as pltpu
from jax.sharding import PartitionSpec as P

floor_share = 0.5
LANES = 128
SUBLANES = 8
HALO = 3
EPS_ROWS = 2
BASE_SUMS = 9
MARK_SUMS = 6
LINE_SUMS = 27
FWD_SUMS = BASE_SUMS + MARK_SUMS
GROUP_LANES = 64
TABLE_COLUMNS = 7
INNER_LIMIT = 2 * 2**20
OUTER_LIMIT = 4 * 2**20
FINISH_LIMIT = 10 * 2**20
VMEM = pl.BlockSpec(memory_space=pltpu.VMEM)
SMEM = pl.BlockSpec(memory_space=pltpu.SMEM)
HBM = pl.BlockSpec(memory_space=pltpu.HBM)


def lane_slice(j):
    return slice(j * LANES, (j + 1) * LANES)


def is_odd(first_row_ref, rows):
    return lax.rem(first_row_ref[0], 2 * rows) != 0


def pack_kernel(first_row_ref, field_ref, *refs, with_eps):
    if with_eps:
        eps_ref, first_ref, second_ref = refs
    else:
        first_ref, second_ref = refs
    waves, parts, rows, width = field_ref.shape
    odd = is_odd(first_row_ref, rows)
    pieces = [
        (slice(wave0, wave0 + SUBLANES), part)
        for wave0 in range(0, waves, SUBLANES)
        for part in range(parts)
    ]
    if with_eps:
        at = HALO * parts * waves
        low = jnp.tile(eps_ref[:EPS_ROWS, :], (SUBLANES // EPS_ROWS, 1))
        high = jnp.tile(eps_ref[rows - EPS_ROWS :, :], (SUBLANES // EPS_ROWS, 1))
        first_ref[at : at + SUBLANES, :] = jnp.where(odd, low, high)
        second_ref[at : at + SUBLANES, :] = jnp.where(odd, high, low)
    for group, part in pieces:
        for lane0 in range(0, width, LANES):
            lanes = slice(lane0, lane0 + LANES)
            head = jnp.swapaxes(field_ref[group, part, :SUBLANES, lanes], 0, 1)
            tail = jnp.swapaxes(field_ref[group, part, rows - SUBLANES :, lanes], 0, 1)
            for k in range(HALO):
                at = (k * parts + part) * waves + group.start
                low = head[k]
                high = tail[SUBLANES - HALO + k]
                first_ref[at : at + SUBLANES, lanes] = jnp.where(odd, low, high)
                second_ref[at : at + SUBLANES, lanes] = jnp.where(odd, high, low)


def outer_rows(first_row, field, eps=None):
    waves, parts, rows, width = field.shape
    height = HALO * parts * waves + (0 if eps is None else SUBLANES)
    shape = jax.ShapeDtypeStruct((height, width), jnp.float32)
    return pl.pallas_call(
        functools.partial(pack_kernel, with_eps=eps is not None),
        in_specs=[SMEM, VMEM] + ([] if eps is None else [VMEM]),
        out_specs=[VMEM, VMEM],
        out_shape=[shape, shape],
        compiler_params=pltpu.CompilerParams(
            vmem_limit_bytes=INNER_LIMIT
        ),
        name="outer_rows",
    )(first_row, field, *(() if eps is None else (eps,)))


def lane_neighbours(load, count):
    lane = lax.broadcasted_iota(jnp.int32, (SUBLANES, LANES), 1)
    at_low = lane == 0
    at_high = lane == LANES - 1
    zero = jnp.zeros((SUBLANES, LANES), jnp.float32)
    tile = load(0)
    up_before = zero
    down_here = pltpu.roll(tile, LANES - 1, 1)
    for j in range(count):
        up_here = pltpu.roll(tile, 1, 1)
        if j + 1 < count:
            following = load(j + 1)
            down_after = pltpu.roll(following, LANES - 1, 1)
        else:
            following, down_after = None, zero
        yield (
            j,
            tile,
            jnp.where(at_low, up_before, up_here) + jnp.where(at_high, down_after, down_here),
        )
        tile, up_before, down_here = following, up_here, down_after


class Scalars:
    def __init__(self, whole_ref, real_ref):
        self.whole, self.real = whole_ref, real_ref
        self.waves = real_ref.shape[0] // 3
        self.first_row = whole_ref[0]

    def source(self, w):
        return self.whole[1 + w]

    def monitor(self, w):
        return self.whole[1 + self.waves + w]

    def squared_k(self, w):
        return self.real[w]

    def cosine(self, w):
        return self.real[self.waves + w]

    def sine(self, w):
        return self.real[2 * self.waves + w]


class Rows:
    def __init__(self, x_ref, z_ref, u_ref, diag_ref, inv_ref, wave_ref):
        self.x, self.z, self.u = x_ref, z_ref, u_ref
        self.diag, self.inv, self.wave = diag_ref, inv_ref, wave_ref
        _, self.parts, self.waves, width = z_ref.shape
        self.rows = z_ref.shape[0] - 4
        self.tiles = width // LANES

    def groups(self):
        return [slice(w, w + SUBLANES) for w in range(0, self.waves, SUBLANES)]

    def column(self, index, group):
        return self.wave[index, group, :]

    def set_diagonal(self, i, eps_row):
        for group in self.groups():
            squared_k = self.column(0, group)
            for j in range(self.tiles):
                lanes = lane_slice(j)
                diagonal = 4.0 - squared_k * jnp.broadcast_to(eps_row(lanes), (SUBLANES, LANES))
                self.diag[i, group, lanes] = diagonal
                self.inv[i, group, lanes] = 1.0 / diagonal

    def tiles_of(self, ref, i, count, group):
        chains = [
            [
                lane_neighbours(
                    lambda j, at=i + k, part=part: ref[at, part, group, lane_slice(j)], self.tiles
                )
                for part in range(self.parts)
            ]
            for k in range(count)
        ]
        for j in range(self.tiles):
            lanes = lane_slice(j)
            now = [[next(chain)[1:] for chain in row] for row in chains]
            out = []
            for k in range(count):
                row = []
                for part in range(self.parts):
                    low = now[k - 1][part][0] if k else ref[i - 1, part, group, lanes]
                    high = now[k + 1][part][0] if k + 1 < count else ref[i + count, part, group, lanes]
                    centre, sides = now[k][part]
                    row.append((centre, low + high, sides))
                out.append(row)
            yield j, out

    def residual(self, i, count):
        for group in self.groups():
            for j, block in self.tiles_of(self.x, i + 1, count, group):
                lanes = lane_slice(j)
                for k in range(count):
                    diagonal = self.diag[i + k, group, lanes]
                    inverse = self.inv[i + k, group, lanes]
                    for part, (centre, around, sides) in enumerate(block[k]):
                        self.z[i + k, part, group, lanes] = (
                            around + sides - diagonal * centre
                        ) * inverse

    def image(self, i, count):
        for group in self.groups():
            for j, block in self.tiles_of(self.z, i + 1, count, group):
                lanes = lane_slice(j)
                for k in range(count):
                    inverse = self.inv[i + 1 + k, group, lanes]
                    for part, (centre, around, sides) in enumerate(block[k]):
                        self.u[i + k, part, group, lanes] = centre - (around + sides) * inverse

    def vectors(self, i, group, count=1):
        for j, block in self.tiles_of(self.u, i + 1, count, group):
            lanes = lane_slice(j)
            for k in range(count):
                diagonal = self.diag[i + 2 + k, group, lanes]
                r, v, w = [], [], []
                for part, (centre, around, sides) in enumerate(block[k]):
                    r.append(diagonal * self.z[i + 2 + k, part, group, lanes])
                    v.append(diagonal * centre)
                    w.append(v[-1] - (around + sides))
                yield j, r, v, w

    def twice(self, i, group, sums, count):
        rr, rv_re, rv_im, vv, wr_re, wr_im, wv_re, wv_im, ww = sums
        for _, r, v, w in self.vectors(i, group, count):
            rr += r[0] * r[0] + r[1] * r[1]
            rv_re += r[0] * v[0] + r[1] * v[1]
            rv_im += r[0] * v[1] - r[1] * v[0]
            vv += v[0] * v[0] + v[1] * v[1]
            wr_re += w[0] * r[0] + w[1] * r[1]
            wr_im += w[0] * r[1] - w[1] * r[0]
            wv_re += w[0] * v[0] + w[1] * v[1]
            wv_im += w[0] * v[1] - w[1] * v[0]
            ww += w[0] * w[0] + w[1] * w[1]
        return rr, rv_re, rv_im, vv, wr_re, wr_im, wv_re, wv_im, ww

    def any_at(self, row_of, row):
        hit = row_of(0) == row
        for w in range(1, self.waves):
            hit = jnp.logical_or(hit, row_of(w) == row)
        return hit

    def source(self, i, scalars, total_rows, side_ref):
        row = scalars.first_row + i - 2
        row = jnp.where(row < 0, row + total_rows, row)
        row = jnp.where(row >= total_rows, row - total_rows, row)

        @pl.when(self.any_at(scalars.source, row))
        def _():
            for group in self.groups():
                cosine, sine = self.frame(i - 2, group)
                chosen = self.column(5, group) == row.astype(jnp.float32)
                for j in range(self.tiles):
                    lanes = lane_slice(j)
                    re = side_ref[group, 0, lanes]
                    im = side_ref[group, 1, lanes]
                    inverse = self.inv[i, group, lanes]
                    self.z[i, 0, group, lanes] += jnp.where(
                        chosen, (cosine * re - sine * im) * inverse, 0.0
                    )
                    self.z[i, 1, group, lanes] += jnp.where(
                        chosen, (sine * re + cosine * im) * inverse, 0.0
                    )

    def frame(self, row, group):
        below = row < 0
        above = row >= self.rows
        return (
            jnp.where(below, self.column(1, group), jnp.where(above, self.column(3, group), 1.0)),
            jnp.where(below, self.column(2, group), jnp.where(above, self.column(4, group), 0.0)),
        )


def wave_column(value_of, wave0):
    sublane = lax.broadcasted_iota(jnp.int32, (SUBLANES, LANES), 0)
    out = jnp.zeros((SUBLANES, LANES), jnp.float32)
    for k in range(SUBLANES):
        out = jnp.where(sublane == k, value_of(wave0 + k).astype(jnp.float32), out)
    return out


def fill_table(table_ref, scalars, rows, total_rows, sign):
    at_first = scalars.first_row == 0
    at_last = scalars.first_row == total_rows - rows
    for wave0 in range(0, table_ref.shape[1], SUBLANES):
        group = slice(wave0, wave0 + SUBLANES)
        cosine = wave_column(scalars.cosine, wave0)
        sine = sign * wave_column(scalars.sine, wave0)
        table_ref[0, group, :] = wave_column(scalars.squared_k, wave0)
        table_ref[1, group, :] = jnp.where(at_first, cosine, 1.0)
        table_ref[2, group, :] = jnp.where(at_first, -sine, 0.0)
        table_ref[3, group, :] = jnp.where(at_last, cosine, 1.0)
        table_ref[4, group, :] = jnp.where(at_last, sine, 0.0)
        table_ref[5, group, :] = wave_column(scalars.source, wave0)
        table_ref[6, group, :] = wave_column(scalars.monitor, wave0)


def lanes_of(out, totals, wave0, offset):
    lane = lax.broadcasted_iota(jnp.int32, (SUBLANES, LANES), 1)
    base = wave0 // SUBLANES * GROUP_LANES + offset
    for n, total in enumerate(totals):
        out = jnp.where(lane == base + n, jnp.sum(total, axis=1, keepdims=True), out)
    return out


def inner_kernel(*refs, forward, total_rows):
    scalars = Scalars(*refs[:2])
    field_ref, refs = refs[2], refs[3:]
    if forward:
        (eps_ref, side_ref) = refs[:2]
        (x_ref, z_ref, u_ref, sums_ref, diag_ref, inv_ref, table_ref) = refs[2:]
    else:
        (diag_ref, inv_ref) = refs[:2]
        (x_ref, z_ref, u_ref, sums_ref, table_ref) = refs[2:]
    step = Rows(x_ref, z_ref, u_ref, diag_ref, inv_ref, table_ref)
    rows, waves = step.rows, step.waves
    fill_table(table_ref, scalars, rows, total_rows, 1.0 if forward else -1.0)
    if forward:
        for row in range(rows):
            step.set_diagonal(row + 2, lambda lanes, row=row: eps_ref[row : row + 1, lanes])
    def turn(j, _):
        lanes = pl.ds(pl.multiple_of(j * LANES, LANES), LANES)
        for part in range(step.parts):
            for group in step.groups():
                for row0 in range(0, rows, SUBLANES):
                    x_ref[HALO + row0 : HALO + row0 + SUBLANES, part, group, lanes] = (
                        jnp.swapaxes(
                            field_ref[group, part, row0 : row0 + SUBLANES, lanes], 0, 1
                        )
                    )
        return 0

    lax.fori_loop(0, step.tiles, turn, 0)

    def residual(t, _):
        i = 3 + 2 * t
        step.residual(i, 2)
        if forward:
            step.source(i, scalars, total_rows, side_ref)
            step.source(i + 1, scalars, total_rows, side_ref)
        return 0

    def image(t, _):
        step.image(3 + 3 * t, 3)
        return 0

    lax.fori_loop(0, (rows - 2) // 2, residual, 0)
    lax.fori_loop(0, (rows - 4) // 3, image, 0)
    zero = jnp.zeros((SUBLANES, LANES), jnp.float32)
    out = zero
    for group in step.groups():
        sums = lax.fori_loop(
            0,
            (rows - 6) // 2,
            lambda t, sums, group=group: step.twice(3 + 2 * t, group, sums, 2),
            (zero,) * BASE_SUMS,
        )
        out = lanes_of(out, sums, group.start, 0 if forward else FWD_SUMS)
    sums_ref[...] = out


def outer_kernel(*refs, forward, total_rows):
    scalars = Scalars(*refs[:2])
    first_ref, second_ref, refs = refs[2], refs[3], refs[4:]
    if forward:
        (part_ref, _, _, _, _, _, side_ref, mark_ref) = refs[:8]
        (x_ref, z_ref, u_ref, diag_ref, inv_ref, sums_ref, table_ref, mark_sums) = refs[8:]
    else:
        (part_ref, _, _, _, diag_ref, inv_ref, line_ref, inner_line_sums, fwd_sums_ref) = refs[:9]
        (x_ref, z_ref, u_ref, sums_ref, table_ref, line_sums) = refs[9:]
    step = Rows(x_ref, z_ref, u_ref, diag_ref, inv_ref, table_ref)
    rows, parts, waves, tiles = step.rows, step.parts, step.waves, step.tiles
    first_row = scalars.first_row
    odd = lax.rem(first_row, 2 * rows) != 0
    fill_table(table_ref, scalars, rows, total_rows, 1.0 if forward else -1.0)
    for group in step.groups():
        for base, offset, swap in ((0, 1, False), (HALO + rows, 3, True)):
            cosine = step.column(offset, group)
            sine = step.column(offset + 1, group)
            for k in range(HALO):
                for j in range(tiles):
                    lanes = lane_slice(j)
                    values = []
                    for part in range(parts):
                        at = (k * parts + part) * waves + group.start
                        one = first_ref[at : at + SUBLANES, lanes]
                        two = second_ref[at : at + SUBLANES, lanes]
                        values.append(jnp.where(odd, two, one) if swap else jnp.where(odd, one, two))
                    re, im = values
                    x_ref[base + k, 0, group, lanes] = cosine * re - sine * im
                    x_ref[base + k, 1, group, lanes] = sine * re + cosine * im
    if forward:
        at = HALO * parts * waves
        for k in range(EPS_ROWS):

            def above_eps(lanes, k=k):
                row = slice(at + k, at + k + 1)
                return jnp.where(odd, first_ref[row, lanes], second_ref[row, lanes])

            def below_eps(lanes, k=k):
                row = slice(at + k, at + k + 1)
                return jnp.where(odd, second_ref[row, lanes], first_ref[row, lanes])

            step.set_diagonal(k, above_eps)
            step.set_diagonal(rows + 2 + k, below_eps)

    def residual(t, _):
        i = t * (rows + 1)
        step.residual(i, 3)
        if forward:
            for k in range(3):
                step.source(i + k, scalars, total_rows, side_ref)
        return 0

    def image(t, _):
        step.image(t * (rows - 1), 3)
        return 0

    lax.fori_loop(0, 2, residual, 0)
    lax.fori_loop(0, 2, image, 0)
    zero = jnp.zeros((SUBLANES, LANES), jnp.float32)
    base_sums = []
    for group in step.groups():
        base_sums.append(
            lax.fori_loop(
                0,
                2,
                lambda t, sums, group=group: step.twice(t * (rows - 3), group, sums, 3),
                (zero,) * BASE_SUMS,
            )
        )
    if forward:
        mark_sums[...] = jnp.zeros_like(mark_sums)

        def mark_at(i, _):
            row = first_row + i

            @pl.when(step.any_at(scalars.monitor, row))
            def _():
                for group in step.groups():
                    chosen = step.column(6, group) == row.astype(jnp.float32)
                    for j in range(tiles):
                        lanes = lane_slice(j)
                        m_re = jnp.where(chosen, mark_ref[group, 0, lanes], 0.0)
                        m_im = jnp.where(chosen, mark_ref[group, 1, lanes], 0.0)
                        for n, (ref, shift) in enumerate(((x_ref, 3), (z_ref, 2), (u_ref, 1))):
                            f_re = ref[i + shift, 0, group, lanes]
                            f_im = ref[i + shift, 1, group, lanes]
                            mark_sums[2 * n, group] += m_re * f_re + m_im * f_im
                            mark_sums[2 * n + 1, group] += m_re * f_im - m_im * f_re

            return 0

        lax.fori_loop(0, rows, mark_at, 0)
        extra, count = mark_sums, MARK_SUMS
    else:
        line_products(
            step,
            scalars,
            total_rows,
            line_ref,
            line_sums,
            lambda row: jnp.logical_and(
                jnp.logical_and(row >= 0, row < rows),
                jnp.logical_or(row < 3, row >= rows - 3),
            ),
        )
        line_sums[...] += inner_line_sums[...]
        extra, count = line_sums, LINE_SUMS
    out = part_ref[...]
    new = jnp.zeros((SUBLANES, LANES), jnp.float32)
    for n, group in enumerate(step.groups()):
        more = list(base_sums[n]) + [extra[k, group] for k in range(count)]
        new = lanes_of(new, more, group.start, 0 if forward else FWD_SUMS)
    out = out + new
    if forward:
        sums_ref[...] = out
    else:
        out = out + fwd_sums_ref[...]
        for n in range(sums_ref.shape[0]):
            sums_ref[n] = out


def distance_to(row, first_row, total_rows):
    away = row - first_row
    away = jnp.where(away >= total_rows - 2, away - total_rows, away)
    return jnp.where(away < -2, away + total_rows, away)


def dot(a, b):
    return a[0] * b[0] + a[1] * b[1], a[0] * b[1] - a[1] * b[0]


def line_waves(step, scalars, total_rows, body):
    def one_wave(w, _):
        away = distance_to(scalars.monitor(w), scalars.first_row, total_rows)

        @pl.when(away <= step.rows + 1)
        def _():
            group = pl.ds(pl.multiple_of((w // SUBLANES) * SUBLANES, SUBLANES), SUBLANES)
            sublane = lax.broadcasted_iota(jnp.int32, (SUBLANES, LANES), 0)
            body(away, group, sublane == w % SUBLANES)

        return 0

    lax.fori_loop(0, step.waves, one_wave, 0)


def line_plane(line_ref, n, part, group, mine):
    return lambda j: jnp.where(mine, line_ref[n, part, group, lane_slice(j)], 0.0)


def line_fields(step, scalars, total_rows, mark_ref, line_ref):
    rows, tiles = step.rows, step.tiles
    line_ref[...] = jnp.zeros_like(line_ref)

    def body(away, group, mine):
        cosine, sine = step.frame(away, group)
        before = jnp.maximum(away + 1, 0)
        after = jnp.minimum(away + 3, rows + 3)
        for j in range(tiles):
            lanes = lane_slice(j)
            m_re = jnp.where(mine, mark_ref[group, 0, lanes], 0.0)
            m_im = jnp.where(mine, mark_ref[group, 1, lanes], 0.0)
            g = (cosine * m_re + sine * m_im, sine * m_re - cosine * m_im)
            for part in range(2):
                z = g[part] * step.inv[away + 2, group, lanes]
                line_ref[0, part, group, lanes] += z
                line_ref[1, part, group, lanes] -= z * step.inv[before, group, lanes]
                line_ref[3, part, group, lanes] -= z * step.inv[after, group, lanes]
                line_ref[4, part, group, lanes] += g[part]
        for part in range(2):
            for j, _, sides in lane_neighbours(line_plane(line_ref, 0, part, group, mine), tiles):
                lanes = lane_slice(j)
                image = line_plane(line_ref, 4, part, group, mine)(j) - sides
                line_ref[5, part, group, lanes] += image
                line_ref[2, part, group, lanes] += image * step.inv[away + 2, group, lanes]

    line_waves(step, scalars, total_rows, body)


def line_products(step, scalars, total_rows, line_ref, line_sums, counts):
    line_sums[...] = jnp.zeros_like(line_sums)

    def body(away, group, mine):
        for k in range(-2, 3):

            @pl.when(counts(away + k))
            def _(k=k):
                zero = jnp.zeros((SUBLANES, LANES), jnp.float32)
                totals = [zero] * LINE_SUMS

                def add(at, pair):
                    totals[at] = totals[at] + pair[0]
                    totals[at + 1] = totals[at + 1] + pair[1]

                if abs(k) < 2:
                    sides_of = [
                        [
                            sides
                            for _, _, sides in lane_neighbours(
                                line_plane(line_ref, 2 + k, part, group, mine), step.tiles
                            )
                        ]
                        for part in range(2)
                    ]
                for j, r, v, w_vec in step.vectors(away + k, group):
                    get = lambda n: [
                        line_plane(line_ref, n, part, group, mine)(j) for part in range(2)
                    ]
                    if abs(k) == 2:
                        wg = [-t for t in get(1 if k < 0 else 3)]
                    elif abs(k) == 1:
                        vg = [-t for t in get(0)]
                        mid = get(2)
                        wg = [vg[p] - mid[p] - sides_of[p][j] for p in range(2)]
                    else:
                        g, vg, low, high = get(4), get(5), get(1), get(3)
                        wg = [vg[p] - (low[p] + high[p]) - sides_of[p][j] for p in range(2)]
                    add(0, dot(wg, r))
                    add(2, dot(wg, v))
                    add(4, dot(w_vec, wg))
                    totals[6] = totals[6] + dot(wg, wg)[0]
                    if abs(k) < 2:
                        add(7, dot(r, vg))
                        add(9, dot(v, vg))
                        add(11, dot(w_vec, vg))
                        add(13, dot(wg, vg))
                        totals[15] = totals[15] + dot(vg, vg)[0]
                    if k == 0:
                        add(16, dot(r, g))
                        add(18, dot(g, v))
                        add(20, dot(g, vg))
                        add(22, dot(w_vec, g))
                        add(24, dot(wg, g))
                        totals[26] = totals[26] + dot(g, g)[0]
                used = 7 if abs(k) == 2 else 16 if abs(k) == 1 else LINE_SUMS
                for n in range(used):
                    line_sums[n, group] += totals[n]

    line_waves(step, scalars, total_rows, body)


def line_kernel(
    whole_ref,
    real_ref,
    z_ref,
    u_ref,
    diag_ref,
    inv_ref,
    mark_ref,
    line_ref,
    line_sums,
    table_ref,
    *,
    total_rows,
):
    scalars = Scalars(whole_ref, real_ref)
    step = Rows(None, z_ref, u_ref, diag_ref, inv_ref, table_ref)
    fill_table(table_ref, scalars, step.rows, total_rows, -1.0)
    line_fields(step, scalars, total_rows, mark_ref, line_ref)
    line_products(
        step,
        scalars,
        total_rows,
        line_ref,
        line_sums,
        lambda row: jnp.logical_and(row >= 3, row < step.rows - 3),
    )


def inner_lines(scalars, z, u, diag, inv, profile, total_rows):
    _, parts, waves, width = z.shape
    return pl.pallas_call(
        functools.partial(line_kernel, total_rows=total_rows),
        in_specs=[SMEM] * 2 + [VMEM] * 5,
        out_specs=[VMEM, VMEM],
        out_shape=[array(6, parts, waves, width), array(LINE_SUMS, waves, LANES)],
        scratch_shapes=[pltpu.VMEM((TABLE_COLUMNS, waves, LANES), jnp.float32)],
        compiler_params=pltpu.CompilerParams(vmem_limit_bytes=INNER_LIMIT),
        name="adjoint_line",
    )(*scalars, z, u, diag, inv, profile)


def array(*shape):
    return jax.ShapeDtypeStruct(shape, jnp.float32)


def inner_rows(forward, field, scalars, extra, total_rows):
    waves, parts, rows, width = field.shape
    args = (*scalars, field, *extra)
    out_shape = [
        array(rows + 6, parts, waves, width),
        array(rows + 4, parts, waves, width),
        array(rows + 2, parts, waves, width),
        array(SUBLANES, LANES),
    ]
    if forward:
        out_shape += [array(rows + 4, waves, width)] * 2
    return pl.pallas_call(
        functools.partial(inner_kernel, forward=forward, total_rows=total_rows),
        in_specs=[SMEM] * 2 + [VMEM, VMEM, VMEM],
        out_specs=[VMEM] * len(out_shape),
        out_shape=out_shape,
        scratch_shapes=[
            pltpu.VMEM((TABLE_COLUMNS, waves, LANES), jnp.float32),
        ],
        compiler_params=pltpu.CompilerParams(
            vmem_limit_bytes=INNER_LIMIT
        ),
        name="forward_inner" if forward else "adjoint_inner",
    )(*args)


def outer_rows_solve(forward, scalars, received, inner, more, copies, total_rows):
    x, z, u, sums, diag, inv = inner
    waves = x.shape[2]
    args = (*scalars, *received, sums, x, z, u, diag, inv, *more)
    scratch = [pltpu.VMEM((TABLE_COLUMNS, waves, LANES), jnp.float32)]
    if forward:
        out_shape = [array(*a.shape) for a in (x, z, u, diag, inv, sums)]
        aliases = {5: 0, 6: 1, 7: 2, 8: 3, 9: 4}
        scratch += [pltpu.VMEM((MARK_SUMS, waves, LANES), jnp.float32)]
    else:
        out_shape = [array(*a.shape) for a in (x, z, u)] + [array(copies, SUBLANES, LANES)]
        aliases = {5: 0, 6: 1, 7: 2}
        scratch += [pltpu.VMEM((LINE_SUMS, waves, LANES), jnp.float32)]
    return pl.pallas_call(
        functools.partial(outer_kernel, forward=forward, total_rows=total_rows),
        in_specs=[SMEM] * 2 + [VMEM] * (len(args) - 2),
        out_specs=[VMEM] * len(out_shape),
        out_shape=out_shape,
        scratch_shapes=scratch,
        input_output_aliases=aliases,
        compiler_params=pltpu.CompilerParams(vmem_limit_bytes=OUTER_LIMIT),
        name="forward_outer" if forward else "adjoint_outer",
    )(*args)


def finish_kernel(
    whole_ref,
    real_ref,
    sums_ref,
    xf_ref,
    zf_ref,
    uf_ref,
    xa_ref,
    _z_in,
    _u_in,
    line_ref,
    fwd_hbm,
    adj_hbm,
    grad_ref,
    za_ref,
    ua_ref,
    coef_ref,
    fwd_stage,
    adj_stage,
    sems,
    *,
    total_rows,
):
    waves, parts, rows, width = fwd_hbm.shape
    tiles = width // LANES
    groups = [slice(w, w + SUBLANES) for w in range(0, waves, SUBLANES)]
    scalars = Scalars(whole_ref, real_ref)

    def column(index, group):
        return coef_ref[index, group, :]

    sums = jnp.sum(sums_ref[...], axis=0)
    for group in groups:
        base = group.start // SUBLANES * GROUP_LANES
        cols = [
            jnp.broadcast_to(sums[:, base + n : base + n + 1], (SUBLANES, LANES))
            for n in range(FWD_SUMS + BASE_SUMS + LINE_SUMS)
        ]
        fwd_coefs = step_lengths(*cols[:BASE_SUMS])
        a_re, a_im, b_re, b_im = fwd_coefs
        s0_re, s0_im, s1_re, s1_im, s2_re, s2_im = cols[BASE_SUMS:FWD_SUMS]
        over_re = s0_re + (a_re * s1_re - a_im * s1_im) + (b_re * s2_re - b_im * s2_im)
        over_im = s0_im + (a_re * s1_im + a_im * s1_re) + (b_re * s2_im + b_im * s2_re)
        adj_cols = cols[FWD_SUMS:]
        adj_coefs = step_lengths(
            *with_line(adj_cols[:BASE_SUMS], adj_cols[BASE_SUMS:], over_re, -over_im)
        )
        twice_k = 2.0 * wave_column(scalars.squared_k, group.start)
        for n, value in enumerate((*fwd_coefs, *adj_coefs, twice_k, over_re, -over_im)):
            coef_ref[n, group, :] = value

    def one_wave(w, _):
        away = distance_to(scalars.monitor(w), scalars.first_row, total_rows)

        @pl.when(away <= rows)
        def _():
            group = pl.ds(pl.multiple_of((w // SUBLANES) * SUBLANES, SUBLANES), SUBLANES)
            mine = lax.broadcasted_iota(jnp.int32, (SUBLANES, LANES), 0) == w % SUBLANES
            b_re = jnp.where(mine, column(9, group), 0.0)
            b_im = jnp.where(mine, column(10, group), 0.0)
            for n, (ref, shift, k) in enumerate(
                ((za_ref, 2, 0), (ua_ref, 1, -1), (ua_ref, 1, 0), (ua_ref, 1, 1))
            ):

                @pl.when(jnp.logical_and(away + k >= 0, away + k < rows))
                def _(n=n, ref=ref, at=away + k + shift):
                    for j in range(tiles):
                        lanes = lane_slice(j)
                        re = line_ref[n, 0, group, lanes]
                        im = line_ref[n, 1, group, lanes]
                        ref[at, 0, group, lanes] += b_re * re - b_im * im
                        ref[at, 1, group, lanes] += b_re * im + b_im * re

        return 0

    lax.fori_loop(0, waves, one_wave, 0)
    sublane = lax.broadcasted_iota(jnp.int32, (SUBLANES, LANES), 0)

    copies = []
    for row0 in range(0, rows, SUBLANES):
        for group in groups:

            def tile_step(j, row0=row0, group=group):
                lanes = pl.ds(pl.multiple_of(j * LANES, LANES), LANES)
                coefs = [column(n, group) for n in range(9)]
                results = [[], [], [], []]
                out = jnp.zeros((SUBLANES, LANES), jnp.float32)
                for k in range(SUBLANES):
                    row = row0 + k
                    values = []
                    for base, x_ref, z_ref, u_ref in (
                        (0, xf_ref, zf_ref, uf_ref),
                        (4, xa_ref, za_ref, ua_ref),
                    ):
                        a_re, a_im, b_re, b_im = coefs[base : base + 4]
                        z_re = z_ref[row + 2, 0, group, lanes]
                        z_im = z_ref[row + 2, 1, group, lanes]
                        u_re = u_ref[row + 1, 0, group, lanes]
                        u_im = u_ref[row + 1, 1, group, lanes]
                        values.append(
                            x_ref[row + HALO, 0, group, lanes]
                            + (a_re * z_re - a_im * z_im)
                            + (b_re * u_re - b_im * u_im)
                        )
                        values.append(
                            x_ref[row + HALO, 1, group, lanes]
                            + (a_re * z_im + a_im * z_re)
                            + (b_re * u_im + b_im * u_re)
                        )
                    f_re, f_im, g_re, g_im = values
                    term = coefs[8] * (g_re * f_re - g_im * f_im)
                    out = jnp.where(sublane == k, jnp.sum(term, axis=0, keepdims=True), out)
                    for n in range(4):
                        results[n].append(values[n])
                for n, (ref, part) in enumerate(
                    ((fwd_stage, 0), (fwd_stage, 1), (adj_stage, 0), (adj_stage, 1))
                ):
                    ref[group, part, row0 : row0 + SUBLANES, lanes] = jnp.swapaxes(
                        jnp.stack(results[n]), 0, 1
                    )
                if group.start:
                    out = out + grad_ref[row0 : row0 + SUBLANES, lanes]
                grad_ref[row0 : row0 + SUBLANES, lanes] = out

            def four_tiles(t, _, tile_step=tile_step):
                for n in range(4):
                    tile_step(4 * t + n)
                return 0

            lax.fori_loop(0, tiles // 4, four_tiles, 0)
            at = pl.ds(group.start, SUBLANES), slice(None), pl.ds(row0, SUBLANES)
            for stage, hbm in ((fwd_stage, fwd_hbm), (adj_stage, adj_hbm)):
                copies.append(pltpu.make_async_copy(stage.at[at], hbm.at[at], sems.at[len(copies)]))
                copies[-1].start()
    for copy in copies:
        copy.wait()


def finish(scalars, sums, forward_parts, adjoint_parts, line, total_rows):
    x, z, u = forward_parts
    rows, parts, waves, width = x.shape[0] - 2 * HALO, *x.shape[1:]
    field = array(waves, parts, rows, width)
    stage = pltpu.VMEM((waves, parts, rows, width), jnp.float32)
    return pl.pallas_call(
        functools.partial(finish_kernel, total_rows=total_rows),
        in_specs=[SMEM] * 2 + [VMEM] * 8,
        out_specs=[HBM, HBM, VMEM, VMEM, VMEM],
        out_shape=[field, field, array(rows, width), array(*z.shape), array(*u.shape)],
        scratch_shapes=[
            pltpu.VMEM((11, waves, LANES), jnp.float32),
            stage,
            stage,
            pltpu.SemaphoreType.DMA((8,)),
        ],
        input_output_aliases={7: 3, 8: 4},
        compiler_params=pltpu.CompilerParams(vmem_limit_bytes=FINISH_LIMIT),
        name="finish",
    )(*scalars, sums, *forward_parts, *adjoint_parts, line)[:3]


def step_lengths(rr, rv_re, rv_im, vv, wr_re, wr_im, wv_re, wv_im, ww):
    half = floor_share * rr
    bounded = jnp.maximum(rv_re * rv_re + rv_im * rv_im, half * half)
    a_re = rr * rv_re / bounded
    a_im = -rr * rv_im / bounded
    a_sq = a_re * a_re + a_im * a_im
    ts_re = rv_re - a_re * vv - (a_re * wr_re + a_im * wr_im) + a_sq * wv_re
    ts_im = -rv_im - a_im * vv - (a_re * wr_im - a_im * wr_re) + a_sq * wv_im
    tt = vv - 2.0 * (a_re * wv_re + a_im * wv_im) + a_sq * ww
    o_re = ts_re / tt
    o_im = ts_im / tt
    return (a_re + o_re, a_im + o_im, a_im * o_im - a_re * o_re, -(a_re * o_im + a_im * o_re))


def with_line(base, line, b_re, b_im):
    rr, rv_re, rv_im, vv, wr_re, wr_im, wv_re, wv_im, ww = base
    b_sq = b_re * b_re + b_im * b_im

    def pair(at):
        return line[at], line[at + 1]

    def times(p):
        return b_re * p[0] - b_im * p[1], b_re * p[1] + b_im * p[0]

    def times_conj(p):
        return b_re * p[0] + b_im * p[1], b_re * p[1] - b_im * p[0]

    def mixed(re, im, forth, back, both):
        f, h = times(forth), times_conj(back)
        return re + f[0] + h[0] + b_sq * both[0], im + f[1] + h[1] + b_sq * both[1]

    def square(value, cross, both):
        return value + 2.0 * times(cross)[0] + b_sq * both

    rv_re, rv_im = mixed(rv_re, rv_im, pair(7), pair(18), pair(20))
    wr_re, wr_im = mixed(wr_re, wr_im, pair(22), pair(0), pair(24))
    wv_re, wv_im = mixed(wv_re, wv_im, pair(11), pair(2), pair(13))
    rr = square(rr, pair(16), line[26])
    vv = square(vv, pair(9), line[15])
    ww = square(ww, pair(4), line[6])
    return rr, rv_re, rv_im, vv, wr_re, wr_im, wv_re, wv_im, ww


def local(
    warm_field,
    warm_adjoint,
    permittivity,
    design_mask,
    source_row,
    monitor_row,
    wavenumber,
    bloch_phase,
    source_profile,
    monitor_profile,
):
    rows = permittivity.shape[0]
    count = lax.axis_size("gx")
    index = lax.axis_index("gx")
    total_rows = rows * count
    first_row = (index * rows).astype(jnp.int32).reshape(1)
    pairing_one = [(i, i ^ 1) for i in range(count)]
    pairing_two = [(i, (i + 1 if i % 2 else i - 1) % count) for i in range(count)]
    fwd_first, fwd_second = outer_rows(first_row, warm_field, permittivity)
    fwd_got = (
        lax.ppermute(fwd_first, "gx", pairing_one),
        lax.ppermute(fwd_second, "gx", pairing_two),
    )
    adj_first, adj_second = outer_rows(first_row, warm_adjoint)
    adj_got = (
        lax.ppermute(adj_first, "gx", pairing_one),
        lax.ppermute(adj_second, "gx", pairing_two),
    )
    scalars = (
        jnp.concatenate([first_row, source_row, monitor_row]),
        jnp.concatenate([wavenumber, jnp.cos(bloch_phase), jnp.sin(bloch_phase)]),
    )
    fx, fz, fu, f_sums, diag, inv = inner_rows(
        True, warm_field, scalars, (permittivity, source_profile), total_rows
    )
    ax, az, au, a_sums = inner_rows(False, warm_adjoint, scalars, (diag, inv), total_rows)
    fx, fz, fu, diag, inv, f_sums = outer_rows_solve(
        True,
        scalars,
        fwd_got,
        (fx, fz, fu, f_sums, diag, inv),
        (source_profile, monitor_profile),
        count,
        total_rows,
    )
    line, line_sums = inner_lines(scalars, az, au, diag, inv, monitor_profile, total_rows)
    ax, az, au, sums = outer_rows_solve(
        False,
        scalars,
        adj_got,
        (ax, az, au, a_sums, diag, inv),
        (line, line_sums, f_sums),
        count,
        total_rows,
    )
    forward, adjoint, partial = finish(
        scalars,
        lax.all_to_all(sums, "gx", 0, 0, tiled=True),
        (fx, fz, fu),
        (ax, az, au),
        line,
        total_rows,
    )
    summed_terms = lax.all_gather(partial, "wa").sum(axis=0)
    gradient = design_mask.astype(jnp.float32) * summed_terms
    return (forward, adjoint, gradient)


def solution(mesh):
    placed = (
        P("wa", None, "gx", None),
        P("wa", None, "gx", None),
        P("gx", None),
        P("gx", None),
        P("wa"),
        P("wa"),
        P("wa"),
        P("wa"),
        P("wa", None, None),
        P("wa", None, None),
    )
    return jax.shard_map(
        local,
        mesh=mesh,
        in_specs=placed,
        out_specs=(P("wa", None, "gx", None), P("wa", None, "gx", None), P("gx", None)),
        check_vma=False,
    )
```
